32 devices in a mesh: gx: 2 (over y), gy: 4 (over x, core), gz: 4 (over z).
Axes of the slice: x: 2, y: 2, z: 4, core: 2. Of those that a mesh axis runs over, the one named last changes fastest.
Arguments:
- residual_in: float32 [2, 8, 32, 512], P('gx', 'gy', 'gz'), may hold values from -6 to 6
- geometry: float32 [3, 2, 8, 32], P(None, 'gx', 'gy', 'gz'), may hold values from 0.5 to 2
- eig_top: float32 [2], replicated, may hold values from 1.5 to 2.5
- coarse_rows: float32 [2, 12, 32, 6, 128], P('gx', 'gy', 'gz'), may hold values from -0.5 to 0.5
- block_ids: int32 [2, 4, 4, 6], P('gx', 'gy', 'gz'), may hold values from 0 to 63, as said below
Outputs:
- correction: float32 [2, 8, 32, 512], P('gx', 'gy', 'gz')
The draws below stay inside these ranges and needn't reach their ends.
Inputs may be any that keep to these rules, and one draw needn't show every extreme that they name: `block_ids`: the 6 ids of one row block are distinct.
All inputs are finite; a program needn't handle non-finite values.
Results may differ from the reference program's by a relative error of at most 0.00018.
Values sent between devices are 32-bit elements; how exact they have to be, the bound alone decides.
No kernel may reach another device: no remote copies, remote signals or barrier semaphores. Data moves between devices by JAX's collectives and lax.ppermute only.
A program may use at most 64 MiB of HBM per device.

```python
import math
import jax
import jax.numpy as jnp
import numpy as np
from jax import lax

CX = 1
CY = 2
CZ = 8
NF = 8
NM = 4
NC = 2
BW = 128
NB = 6
EXT = 2
EYT = 8
EZT = 32
VY = 12
N_GX = 2
N_GY = 4
N_GZ = 4
DEVICES = 32


def draw_block_ids(key, part):
    leaf_key = jax.random.fold_in(key, 17)
    label_key = jax.random.fold_in(key, 29)
    leaves = jax.random.permutation(leaf_key, DEVICES).astype(jnp.int32).reshape(N_GX, N_GY, N_GZ, 1)
    levels = jnp.arange(1, NB, dtype=jnp.int32).reshape(1, 1, 1, NB - 1)
    shared = DEVICES - 1 + jnp.right_shift(DEVICES + leaves, levels)
    layout = jnp.concatenate([leaves, jnp.broadcast_to(shared, (N_GX, N_GY, N_GZ, NB - 1))], axis=3)
    labels = jax.random.permutation(label_key, 2 * DEVICES).astype(jnp.int32)
    return labels[layout]


def level_of(rng, dims, split, low, largest):
    def one(dim, blocks):
        steps = jax.random.uniform(jax.random.fold_in(jax.random.fold_in(rng, 6), dim), (blocks,), jnp.float32, low / len(split), largest / len(split))
        return jnp.repeat(jnp.exp(steps), dims[dim] // blocks).reshape((-1,) + (1,) * (len(dims) - dim - 1))

    factor_of = one(*split[0])
    for cut in split[1:]:
        factor_of = factor_of * one(*cut)
    return factor_of


def noise(own_key, shape, scale, most, shards=(), kind=jnp.bfloat16):
    values = scale * jax.random.normal(own_key, shape, jnp.float32)
    if shards:
        values = values * level_of(own_key, shape, shards, -0.22, 0.18)
    return jnp.clip(values, -most, most).astype(kind)


def setup_inputs(seed: int = 0) -> dict:
    streams_of = jax.random.split(jax.random.key(seed), 6)
    residual_in = noise(streams_of[0], (EXT, EYT, EZT, NF ** 3), 1.0, 6.0, ((0, 2), (1, 4), (2, 4)), jnp.float32)
    geometry = jnp.clip(jnp.exp(math.log(2.0) - 1.3862944 * jax.random.uniform(streams_of[1], (3, EXT, EYT, EZT), jnp.float32) ** level_of(streams_of[1], (3, EXT, EYT, EZT), ((1, 2), (2, 4), (3, 4)), -0.2, 0.2)), 0.5, 2.0)
    eig_top = jnp.clip(jax.random.uniform(streams_of[2], (2,), jnp.float32, 1.5, 2.5), 1.5, 2.5)
    coarse_rows = noise(streams_of[3], (EXT, VY, EZT, NB, BW), (0.7 * (2 * BW * CX * (CY + 1) * CZ * DEVICES) ** -0.25), 0.5, ((0, 2), (1, 4), (2, 4)), jnp.float32)
    block_ids = draw_block_ids(jax.random.fold_in(streams_of[5], 71), 0)
    return dict(residual_in=residual_in, geometry=geometry, eig_top=eig_top, coarse_rows=coarse_rows, block_ids=block_ids)


FULL_PRECISION = lax.Precision.HIGHEST


def legendre_pair(point, degree):
    previous = 1.0
    current = point
    for order in range(1, degree):
        following = ((2 * order + 1) * point * current - order * previous) / (order + 1)
        previous = current
        current = following
    return current, previous


def gll_tables(points):
    degree = points - 1
    node_list = []
    for index in range(points):
        guess = -math.cos(math.pi * index / degree)
        for sweep in range(100):
            high_val, low_val = legendre_pair(guess, degree)
            guess = guess - (guess * high_val - low_val) / (points * high_val)
        node_list.append(guess)
    node_list[0] = -1.0
    node_list[degree] = 1.0
    node_pos = np.array(node_list)
    at_nodes = np.array([legendre_pair(value, degree)[0] for value in node_list])
    weights = 2.0 / (degree * (degree + 1) * at_nodes ** 2)
    derivative = np.zeros((points, points))
    for row_pos in range(points):
        for col_pos in range(points):
            if row_pos != col_pos:
                derivative[row_pos, col_pos] = at_nodes[row_pos] / (at_nodes[col_pos] * (node_pos[row_pos] - node_pos[col_pos]))
    derivative[0, 0] = -degree * (degree + 1) / 4.0
    derivative[degree, degree] = degree * (degree + 1) / 4.0
    stiffness = derivative.T @ (weights[:, None] * derivative)
    return node_pos, weights, stiffness


def interp_table(fine_pts, coarse_pts):
    fine_nodes = gll_tables(fine_pts)[0]
    coarse_nodes = gll_tables(coarse_pts)[0]
    lagrange = np.ones((fine_pts, coarse_pts))
    for col_pos in range(coarse_pts):
        for other_pos in range(coarse_pts):
            if other_pos != col_pos:
                lagrange[:, col_pos] *= (fine_nodes - coarse_nodes[other_pos]) / (coarse_nodes[col_pos] - coarse_nodes[other_pos])
    return lagrange


def level_tables(points):
    node_pos, weights, stiffness = gll_tables(points)
    return jnp.asarray(weights, jnp.float32), jnp.asarray(stiffness, jnp.float32)


def local_apply(nodal, coeffs, weights, stiffness):
    plane_w = weights[:, None] * weights[None, :]
    term_x = jnp.einsum('ia,...abc->...ibc', stiffness, nodal, precision=FULL_PRECISION) * plane_w
    term_y = jnp.einsum('jb,...abc->...ajc', stiffness, nodal, precision=FULL_PRECISION) * plane_w[:, None, :]
    term_z = jnp.einsum('kc,...abc->...abk', stiffness, nodal, precision=FULL_PRECISION) * plane_w[:, :, None]
    return coeffs[0][..., None, None, None] * term_x + coeffs[1][..., None, None, None] * term_y + coeffs[2][..., None, None, None] * term_z


def local_diagonal(coeffs, weights, stiffness):
    stiff_diag = jnp.diag(stiffness)
    part_x = stiff_diag[:, None, None] * weights[None, :, None] * weights[None, None, :]
    part_y = weights[:, None, None] * stiff_diag[None, :, None] * weights[None, None, :]
    part_z = weights[:, None, None] * weights[None, :, None] * stiff_diag[None, None, :]
    return coeffs[0][..., None, None, None] * part_x + coeffs[1][..., None, None, None] * part_y + coeffs[2][..., None, None, None] * part_z


def chebyshev(residual, initial, top_eig, operate, inverse_diag):
    center = 0.55 * top_eig
    spread_eig = 0.45 * top_eig
    sigma_ratio = center / spread_eig
    rho_first = 1.0 / sigma_ratio
    rho_next = 1.0 / (2.0 * sigma_ratio - rho_first)
    if initial is None:
        current = residual
    else:
        current = residual - operate(initial)
    step_one = inverse_diag * current / center
    iterate = step_one if initial is None else initial + step_one
    second_res = residual - operate(iterate)
    step_two = rho_first * rho_next * step_one + (2.0 * rho_next / spread_eig) * (inverse_diag * second_res)
    return iterate + step_two


def prolong(nodal, lagrange):
    nodal = jnp.einsum('ia,...abc->...ibc', lagrange, nodal, precision=FULL_PRECISION)
    nodal = jnp.einsum('jb,...abc->...ajc', lagrange, nodal, precision=FULL_PRECISION)
    return jnp.einsum('kc,...abc->...abk', lagrange, nodal, precision=FULL_PRECISION)


def restrict(nodal, lagrange):
    nodal = jnp.einsum('ia,...ibc->...abc', lagrange, nodal, precision=FULL_PRECISION)
    nodal = jnp.einsum('jb,...ajc->...abc', lagrange, nodal, precision=FULL_PRECISION)
    return jnp.einsum('kc,...abk->...abc', lagrange, nodal, precision=FULL_PRECISION)


def multiplicity(points, elem_y, total_y):
    degree = points - 1
    first_node = (jnp.arange(points) == 0).astype(jnp.float32)
    last_node = (jnp.arange(points) == degree).astype(jnp.float32)
    side_x = 1.0 + first_node + last_node
    low_flag = (elem_y > 0).astype(jnp.float32)
    high_flag = (elem_y < total_y - 1).astype(jnp.float32)
    side_y = 1.0 + low_flag[:, None] * first_node[None, :] + high_flag[:, None] * last_node[None, :]
    return side_x[None, None, None, :, None, None] * side_y[None, :, None, None, :, None] * side_x[None, None, None, None, None, :]


def ref_pass(nodal, direction, periodic):
    dim_count = nodal.ndim
    elem_axis = dim_count - 6 + direction
    point_axis = dim_count - 3 + direction
    degree = nodal.shape[point_axis] - 1
    left_face = jnp.take(nodal, 0, axis=point_axis)
    right_face = jnp.take(nodal, degree, axis=point_axis)
    summed = right_face + jnp.roll(left_face, -1, axis=elem_axis)
    before = jnp.roll(summed, 1, axis=elem_axis)
    if not periodic:
        extent = nodal.shape[elem_axis]
        shape_list = [1] * left_face.ndim
        shape_list[elem_axis] = extent
        where_pos = jnp.arange(extent).reshape(shape_list)
        summed = jnp.where(where_pos == extent - 1, right_face, summed)
        before = jnp.where(where_pos == 0, left_face, before)
    middle = lax.slice_in_dim(nodal, 1, degree, axis=point_axis)
    return jnp.concatenate([jnp.expand_dims(before, point_axis), middle, jnp.expand_dims(summed, point_axis)], axis=point_axis)


def direct_sum(nodal):
    nodal = ref_pass(nodal, 0, True)
    nodal = ref_pass(nodal, 1, False)
    return ref_pass(nodal, 2, True)


def ref_coarse(low_res, coarse_rows, block_ids):
    flat_nodes = low_res.reshape(EXT, EYT, EZT, NC ** 3)
    top_mask = jnp.arange(N_GY) == N_GY - 1
    base_vals = flat_nodes[..., 0].reshape(EXT, N_GY, CY, EZT)
    upper_side = flat_nodes[..., 2].reshape(EXT, N_GY, CY, EZT)[:, :, CY - 1:, :]
    upper_side = jnp.where(top_mask[None, :, None, None], upper_side, 0.0)
    owned_vals = jnp.concatenate([base_vals, upper_side], axis=2).reshape(N_GX, CX, N_GY, CY + 1, N_GZ, CZ)
    row_tiles = coarse_rows.reshape(N_GX, CX, N_GY, CY + 1, N_GZ, CZ, NB, BW)
    contrib = jnp.einsum('aibjck,aibjcknw->abcnw', owned_vals, row_tiles, precision=FULL_PRECISION)
    column = jnp.zeros((2 * DEVICES, BW), jnp.float32).at[block_ids.reshape(-1)].add(contrib.reshape(-1, BW))
    picked = column[block_ids]
    solved = jnp.einsum('aibjcknw,abcnw->aibjck', row_tiles, picked, precision=FULL_PRECISION)
    solved = solved.reshape(EXT, N_GY, CY + 1, EZT)
    top_values = jnp.where(top_mask[None, :, None, None], solved[:, :, CY:, :], 0.0)
    zeros_y = jnp.zeros((EXT, N_GY, CY - 1, EZT), jnp.float32)
    corner_two = jnp.concatenate([zeros_y, top_values], axis=2).reshape(EXT, EYT, EZT)
    corner_zero = solved[:, :, :CY, :].reshape(EXT, EYT, EZT)
    zero_nodes = jnp.zeros_like(corner_zero)
    spread = jnp.stack([corner_zero, zero_nodes, corner_two, zero_nodes, zero_nodes, zero_nodes, zero_nodes, zero_nodes], axis=-1)
    return direct_sum(spread.reshape(EXT, EYT, EZT, NC, NC, NC))


def reference(residual_in, geometry, eig_top, coarse_rows, block_ids):
    fine_w, fine_k = level_tables(NF)
    mid_w, mid_k = level_tables(NM)
    up_mid = jnp.asarray(interp_table(NF, NM), jnp.float32)
    up_low = jnp.asarray(interp_table(NM, NC), jnp.float32)
    elem_y = jnp.arange(EYT)
    source = residual_in.reshape(EXT, EYT, EZT, NF, NF, NF)
    stacked = direct_sum(jnp.stack([source, local_diagonal(geometry, fine_w, fine_k)]))
    fine_res = stacked[0]
    fine_inv = 1.0 / stacked[1]

    def fine_op(nodal):
        return direct_sum(local_apply(nodal, geometry, fine_w, fine_k))

    def mid_op(nodal):
        return direct_sum(local_apply(nodal, geometry, mid_w, mid_k))

    fine_x = chebyshev(fine_res, None, eig_top[0], fine_op, fine_inv)
    fine_left = fine_res - fine_op(fine_x)
    mid_src = restrict(fine_left / multiplicity(NF, elem_y, EYT), up_mid)
    stacked = direct_sum(jnp.stack([mid_src, local_diagonal(geometry, mid_w, mid_k)]))
    mid_res = stacked[0]
    mid_inv = 1.0 / stacked[1]
    mid_x = chebyshev(mid_res, None, eig_top[1], mid_op, mid_inv)
    mid_left = mid_res - mid_op(mid_x)
    low_res = direct_sum(restrict(mid_left / multiplicity(NM, elem_y, EYT), up_low))
    low_u = ref_coarse(low_res, coarse_rows, block_ids)
    mid_x = chebyshev(mid_res, mid_x + prolong(low_u, up_low), eig_top[1], mid_op, mid_inv)
    fine_x = chebyshev(fine_res, fine_x + prolong(mid_x, up_mid), eig_top[0], fine_op, fine_inv)
    return fine_x.reshape(EXT, EYT, EZT, NF ** 3)
```

```python
import functools
import math

import jax
import jax.numpy as jnp
import numpy as np
from jax import lax
from jax.experimental import pallas as pl
from jax.experimental.pallas import tpu as pltpu
from jax.sharding import PartitionSpec as P

NF = 8
NM = 4
NC = 2
LANES = 128
SUB = 8
SIGMA = 0.55 / 0.45
RHO0 = 1.0 / SIGMA
RHO1 = 1.0 / (2.0 * SIGMA - RHO0)


def legendre_pair(point, degree):
    previous = 1.0
    current = point
    for order in range(1, degree):
        following = ((2 * order + 1) * point * current - order * previous) / (order + 1)
        previous = current
        current = following
    return (current, previous)


def gll_tables(points):
    degree = points - 1
    node_list = []
    for index in range(points):
        guess = -math.cos(math.pi * index / degree)
        for sweep in range(100):
            high_val, low_val = legendre_pair(guess, degree)
            guess = guess - (guess * high_val - low_val) / (points * high_val)
        node_list.append(guess)
    node_list[0] = -1.0
    node_list[degree] = 1.0
    node_pos = np.array(node_list)
    at_nodes = np.array([legendre_pair(value, degree)[0] for value in node_list])
    weights = 2.0 / (degree * (degree + 1) * at_nodes**2)
    derivative = np.zeros((points, points))
    for row_pos in range(points):
        for col_pos in range(points):
            if row_pos != col_pos:
                derivative[row_pos, col_pos] = at_nodes[row_pos] / (
                    at_nodes[col_pos] * (node_pos[row_pos] - node_pos[col_pos])
                )
    derivative[0, 0] = -degree * (degree + 1) / 4.0
    derivative[degree, degree] = degree * (degree + 1) / 4.0
    stiffness = derivative.T @ (weights[:, None] * derivative)
    return (node_pos, weights, stiffness)


def interp_table(fine_pts, coarse_pts):
    fine_nodes = gll_tables(fine_pts)[0]
    coarse_nodes = gll_tables(coarse_pts)[0]
    lagrange = np.ones((fine_pts, coarse_pts))
    for col_pos in range(coarse_pts):
        for other_pos in range(coarse_pts):
            if other_pos != col_pos:
                lagrange[:, col_pos] *= (fine_nodes - coarse_nodes[other_pos]) / (
                    coarse_nodes[col_pos] - coarse_nodes[other_pos]
                )
    return lagrange


class Level:
    def __init__(self, points):
        self.n = points
        _, weights, stiffness = gll_tables(points)
        self.w = [float(v) for v in weights]
        self.kd = [float(v) for v in np.diag(stiffness)]
        scaled = stiffness / weights[:, None]
        half = points // 2
        flipped = scaled[:, ::-1]
        self.even = [[float(v) for v in row[:half]] for row in (scaled + flipped)[:half] / 2]
        self.odd = [[float(v) for v in row[:half]] for row in (scaled - flipped)[:half] / 2]
        self.scaled = scaled
        self.weights = weights
        self.diag = np.diag(stiffness)


FINE = Level(NF)
MID = Level(NM)
UP_F = interp_table(NF, NM)
UP_C = interp_table(NM, NC)


def shared_faces(lagrange):
    out = lagrange.copy()
    out[0] *= 0.5
    out[-1] *= 0.5
    return out


def pad_rows(column, fill=0.0):
    out = np.full((SUB,), fill)
    out[: column.shape[0]] = column
    return out


def build_tables():
    rows = []
    index = {}

    def put(name, columns):
        index[name] = len(rows)
        rows.extend(columns)

    put("kz8", [FINE.scaled[:, c] for c in range(NF)])
    put("kz4", [pad_rows(MID.scaled[:, c]) for c in range(NM)])
    put("w8", [FINE.weights])
    put("w4", [pad_rows(MID.weights, 1.0)])
    put("kd8", [FINE.diag])
    put("kd4", [pad_rows(MID.diag, 1.0)])
    put("rz8", [pad_rows(shared_faces(UP_F)[c]) for c in range(NF)])
    put("rz4", [pad_rows(shared_faces(UP_C)[c]) for c in range(NM)])
    put("pz8", [UP_F[:, c] for c in range(NM)])
    put("pz4", [pad_rows(UP_C[:, c]) for c in range(NC)])
    flat = np.concatenate(rows).astype(np.float32)
    return np.ascontiguousarray(np.broadcast_to(flat[:, None], (flat.shape[0], LANES))), index


TABLE, TINDEX = build_tables()
MASK_Y_LO, MASK_Y_HI, MASK_Z_LO, MASK_Z_HI, FAC_Y_LO, FAC_Y_HI, DEV_ID, TOP_ROW = range(8)


class Geo:
    def __init__(self, gx, gy, cy, cz, nz):
        self.gx, self.gy, self.cy, self.cz, self.nz = gx, gy, cy, cz, nz
        self.wy = gy * cy
        self.lanes = gx * self.wy * cz
        self.ne = cy * cz
        self.planes = gx * gy
        self.half = gy // 2 if gy % 2 == 0 else gy
        self.cores = gy // self.half
        self.chunks = self.lanes // LANES

    def masks(self):
        lane = np.arange(self.lanes)
        z = lane % self.cz
        y = (lane // self.cz) % self.wy
        out = np.zeros((8, self.lanes), np.float32)
        out[MASK_Y_LO] = y > 0
        out[MASK_Y_HI] = y < self.wy - 1
        out[MASK_Z_LO] = z > 0
        out[MASK_Z_HI] = z < self.cz - 1
        out[FAC_Y_LO] = np.where(y > 0, 0.5, 1.0)
        out[FAC_Y_HI] = np.where(y < self.wy - 1, 0.5, 1.0)
        out[DEV_ID] = lane // self.ne
        out[TOP_ROW] = y == self.wy - 1
        return out


def roll(value, shift):
    size = value.shape[-1]
    shift %= size
    return value if shift == 0 else pltpu.roll(value, shift, axis=value.ndim - 1)


def tab(tref, name, pos=0):
    return tref[pl.ds((TINDEX[name] + pos) * SUB, SUB), :]


def lane_ds(chunk):
    if isinstance(chunk, int):
        return pl.ds(chunk * LANES, LANES)
    return pl.ds(pl.multiple_of(chunk * LANES, LANES), LANES)


def for_tiles(geo, body):
    def step(pos, carry):
        if geo.chunks == 1:
            body(pos, 0)
        else:
            body(pos // geo.chunks, pos % geo.chunks)
        return carry

    lax.fori_loop(0, geo.nz * geo.chunks, step, 0)


def loop(count, body):
    def step(pos, carry):
        body(pos)
        return carry

    lax.fori_loop(0, count, step, 0)


def rows8(pos):
    if isinstance(pos, int):
        return pl.ds(pos * SUB, SUB)
    return pl.ds(pl.multiple_of(pos * SUB, SUB), SUB)


def wide_load(ref, zb, rows, geo):
    parts = [ref[zb, ch, rows, :] for ch in range(geo.chunks)]
    return parts[0] if len(parts) == 1 else jnp.concatenate(parts, axis=1)


def wide_store(ref, zb, rows, geo, value):
    for ch in range(geo.chunks):
        ref[zb, ch, rows, :] = value[:, ch * LANES : (ch + 1) * LANES]


def gather_sum(ref, mref, geo, n):
    xs = geo.wy * geo.cz
    last = (n - 1) * n
    for b in range(n):
        for zb in range(geo.nz):
            low = wide_load(ref, zb, rows8(b), geo)
            high = wide_load(ref, zb, rows8(last + b), geo)
            wide_store(ref, zb, rows8(b), geo, low + roll(high, xs))
            wide_store(ref, zb, rows8(last + b), geo, high + roll(low, -xs))
    y_lo = mref[MASK_Y_LO : MASK_Y_LO + 1, :]
    y_hi = mref[MASK_Y_HI : MASK_Y_HI + 1, :]
    for a in range(n):
        first, final = rows8(a * n), rows8(a * n + n - 1)
        for zb in range(geo.nz):
            low = wide_load(ref, zb, first, geo)
            high = wide_load(ref, zb, final, geo)
            wide_store(ref, zb, first, geo, low + y_lo * roll(high, geo.cz))
            wide_store(ref, zb, final, geo, high + y_hi * roll(low, -geo.cz))
    z_lo = mref[MASK_Z_LO : MASK_Z_LO + 1, :] > 0.5
    z_hi = mref[MASK_Z_HI : MASK_Z_HI + 1, :] > 0.5
    group = min(SUB, n * n)
    for g in range(n * n // group):
        first = pl.ds(g * group * SUB, group, stride=SUB)
        final = pl.ds(g * group * SUB + n - 1, group, stride=SUB)
        low = [wide_load(ref, zb, first, geo) for zb in range(geo.nz)]
        high = [wide_load(ref, zb, final, geo) for zb in range(geo.nz)]
        for zb in range(geo.nz):
            before = roll(high[(zb - 1) % geo.nz], -(geo.cz - 1))
            after = roll(low[(zb + 1) % geo.nz], geo.cz - 1)
            near = jnp.where(z_lo, roll(high[zb], 1), before)
            wide_store(ref, zb, first, geo, low[zb] + near)
            near = jnp.where(z_hi, roll(low[zb], -1), after)
            wide_store(ref, zb, final, geo, high[zb] + near)


def contract(values, level):
    half = level.n // 2
    sums = [values[a] + values[level.n - 1 - a] for a in range(half)]
    diffs = [values[a] - values[level.n - 1 - a] for a in range(half)]
    out = [None] * level.n
    for i in range(half):
        even = sums[0] * level.even[i][0]
        odd = diffs[0] * level.odd[i][0]
        for a in range(1, half):
            even = even + sums[a] * level.even[i][a]
            odd = odd + diffs[a] * level.odd[i][a]
        out[i] = even + odd
        out[level.n - 1 - i] = even - odd
    return out


def combine(values, table):
    out = []
    for i in range(table.shape[0]):
        total = values[0] * float(table[i, 0])
        for a in range(1, table.shape[1]):
            total = total + values[a] * float(table[i, a])
        out.append(total)
    return out


def sublane_mix(ref, zb, ch, row, columns):
    total = ref[zb, ch, pl.ds(row, 1), :] * columns[0]
    for c in range(1, len(columns)):
        total = total + ref[zb, ch, pl.ds(row + c, 1), :] * columns[c]
    return total


def apply_local(src, dst, gref, tref, geo, level):
    n = level.n
    kname, wname = ("kz8", "w8") if n == NF else ("kz4", "w4")

    def body(zb, ch):
        ln = lane_ds(ch)
        wc = tab(tref, wname)
        gw = [gref[zb, ch, pl.ds(i, 1), :] * wc for i in range(3)]
        columns = [tab(tref, kname, c) for c in range(n)]
        for b in range(n):
            mixed = contract([src[zb, ch, rows8(a * n + b), :] for a in range(n)], level)
            for a in range(n):
                dst[zb, ch, rows8(a * n + b), :] = mixed[a] * gw[0]
        for a in range(n):
            mixed = contract([src[zb, ch, rows8(a * n + b), :] for b in range(n)], level)
            for b in range(n):
                row = (a * n + b) * SUB
                along = sublane_mix(src, zb, ch, row, columns)
                total = dst[zb, ch, rows8(a * n + b), :] + mixed[b] * gw[1] + along * gw[2]
                dst[zb, ch, rows8(a * n + b), :] = total * (level.w[a] * level.w[b])

    for_tiles(geo, body)


def local_diagonal(dst, gref, tref, geo, level):
    n = level.n
    wname, dname = ("w8", "kd8") if n == NF else ("w4", "kd4")

    def body(zb, ch):
        ln = lane_ds(ch)
        wc = tab(tref, wname)
        gx = gref[zb, ch, pl.ds(0, 1), :] * wc
        gy = gref[zb, ch, pl.ds(1, 1), :] * wc
        gz = gref[zb, ch, pl.ds(2, 1), :] * tab(tref, dname)
        for a in range(n):
            for b in range(n):
                dst[zb, ch, rows8(a * n + b), :] = (
                    gx * (level.kd[a] * level.w[b])
                    + gy * (level.w[a] * level.kd[b])
                    + gz * (level.w[a] * level.w[b])
                )

    for_tiles(geo, body)


def each_row(geo, n, body):
    def tile(zb, ch):
        for row in range(n * n):
            body(zb, ch, rows8(row))

    for_tiles(geo, tile)


def first_smooth(res, inv, cur, tmp, mref, gref, tref, geo, level, top):
    first = 1.0 / (0.55 * top)
    second = 2.0 * RHO1 / (0.45 * top)

    def start(zb, ch, row):
        value = 1.0 / tmp[zb, ch, row, :]
        inv[zb, ch, row, :] = value
        cur[zb, ch, row, :] = value * res[zb, ch, row, :] * first

    each_row(geo, level.n, start)
    apply_local(cur, tmp, gref, tref, geo, level)
    gather_sum(tmp, mref, geo, level.n)

    def finish(zb, ch, row):
        left = res[zb, ch, row, :] - tmp[zb, ch, row, :]
        cur[zb, ch, row, :] = (1.0 + RHO0 * RHO1) * cur[zb, ch, row, :] + second * (
            inv[zb, ch, row, :] * left
        )

    each_row(geo, level.n, finish)
    apply_local(cur, tmp, gref, tref, geo, level)
    gather_sum(tmp, mref, geo, level.n)


def next_smooth(res, inv, cur, step, tmp, mref, gref, tref, geo, level, top):
    first = 1.0 / (0.55 * top)
    second = 2.0 * RHO1 / (0.45 * top)
    apply_local(cur, tmp, gref, tref, geo, level)
    gather_sum(tmp, mref, geo, level.n)

    def start(zb, ch, row):
        value = inv[zb, ch, row, :] * (res[zb, ch, row, :] - tmp[zb, ch, row, :]) * first
        step[zb, ch, row, :] = value
        cur[zb, ch, row, :] = cur[zb, ch, row, :] + value

    each_row(geo, level.n, start)
    apply_local(cur, tmp, gref, tref, geo, level)
    gather_sum(tmp, mref, geo, level.n)

    def finish(zb, ch, row):
        left = res[zb, ch, row, :] - tmp[zb, ch, row, :]
        cur[zb, ch, row, :] = (
            cur[zb, ch, row, :]
            + (RHO0 * RHO1) * step[zb, ch, row, :]
            + second * (inv[zb, ch, row, :] * left)
        )

    each_row(geo, level.n, finish)


def restrict(res, tmp, dst, mref, tref, geo, nf, nc, table, name, buf):
    scaled = shared_faces(table)

    def body(zb, ch):
        ln = lane_ds(ch)
        f_lo = mref[FAC_Y_LO : FAC_Y_LO + 1, ln]
        f_hi = mref[FAC_Y_HI : FAC_Y_HI + 1, ln]
        part = []
        for b in range(nf):
            values = []
            for a in range(nf):
                row = rows8(a * nf + b)
                values.append(res[zb, ch, row, :] - tmp[zb, ch, row, :])
            mixed = combine(values, scaled.T)
            if b == 0:
                mixed = [v * f_lo for v in mixed]
            if b == nf - 1:
                mixed = [v * f_hi for v in mixed]
            part.append(mixed)
        columns = [tab(tref, name, c) for c in range(nf)]
        for i in range(nc):
            along = combine([part[b][i] for b in range(nf)], table.T)
            for j in range(nc):
                buf[0, 0, rows8(i * nc + j), :] = along[j]
        for row in range(nc * nc):
            dst[zb, ch, rows8(row), :] = sublane_mix(buf, 0, 0, row * SUB, columns)

    for_tiles(geo, body)


def prolong_add(src, cur, tref, geo, nf, nc, table, name):
    def body(zb, ch):
        ln = lane_ds(ch)
        columns = [tab(tref, name, c) for c in range(nc)]
        part = []
        for a in range(nc):
            deep = [
                sublane_mix(src, zb, ch, (a * nc + b) * SUB, columns) for b in range(nc)
            ]
            part.append(combine(deep, table))
        for b in range(nf):
            mixed = combine([part[a][b] for a in range(nc)], table)
            for a in range(nf):
                row = rows8(a * nf + b)
                cur[zb, ch, row, :] = cur[zb, ch, row, :] + mixed[a]

    for_tiles(geo, body)


def split(value):
    high = value.astype(jnp.bfloat16)
    return high, (value - high.astype(jnp.float32)).astype(jnp.bfloat16)


def dot(left, right, dims):
    return lax.dot_general(left, right, (dims, ((), ())), preferred_element_type=jnp.float32)


def dot3(left, right_high, right_low, dims):
    high, low = split(left)
    return dot(high, right_high, dims) + (dot(high, right_low, dims) + dot(low, right_high, dims))


def down_kernel(
    own, par, eig, mref, tref, *refs, geo, nblk, prow
):
    res, inv, cur, resm, invm, curm, gref, xhi, xlo, send, tmp, tmpm, low, buf = refs
    my_x = lax.axis_index("gx")
    my_y = lax.axis_index("gy")
    my_h = my_y // geo.cores
    my_c = my_y % geo.cores

    def piece(ix, iy, start, size):
        rel = lax.rem(ix - my_x + geo.gx, geo.gx) * geo.half + lax.rem(
            iy // geo.cores - my_h + geo.half, geo.half
        )
        mine = own[rel, pl.ds(start, size), :]
        if geo.cores == 1:
            return mine
        return jnp.where(my_c == iy % geo.cores, mine, par[rel, pl.ds(start, size), :])

    devices = [(ix, iy) for ix in range(geo.gx) for iy in range(geo.gy)]
    per_chunk = LANES // geo.ne
    words = NF**3 // LANES
    for zb in range(geo.nz):
        for ch in range(geo.chunks):
            group = devices[ch * per_chunk : (ch + 1) * per_chunk]
            for blk in range(words):
                rows = [piece(ix, iy, zb * prow + blk * geo.ne, geo.ne) for ix, iy in group]
                square = jnp.concatenate(rows, axis=0)
                res[zb, ch, pl.ds(blk * LANES, LANES), :] = square.T
            total = None
            for pos, (ix, iy) in enumerate(group):
                part = roll(piece(ix, iy, zb * prow + words * geo.ne, SUB), pos * geo.ne)
                total = part if total is None else total + part
            gref[zb, ch] = total
    start = geo.nz * prow
    slots = (geo.cy + 1) * geo.cz
    for k in range(nblk):
        base = [piece(ix, iy, start + k * slots, geo.ne) for ix, iy in devices]
        extra = []
        for ix in range(geo.gx):
            extra.append(jnp.zeros(((geo.wy - 1) * geo.cz, LANES), jnp.float32))
            extra.append(piece(ix, geo.gy - 1, start + k * slots + geo.ne, geo.cz))
        high, rest = split(jnp.concatenate(base + extra, axis=0))
        xhi[k] = high
        xlo[k] = rest

    gather_sum(res, mref, geo, NF)
    local_diagonal(tmp, gref, tref, geo, FINE)
    gather_sum(tmp, mref, geo, NF)
    first_smooth(res, inv, cur, tmp, mref, gref, tref, geo, FINE, eig[0])
    restrict(res, tmp, resm, mref, tref, geo, NF, NM, UP_F, "rz8", buf)
    gather_sum(resm, mref, geo, NM)
    local_diagonal(tmpm, gref, tref, geo, MID)
    gather_sum(tmpm, mref, geo, NM)
    first_smooth(resm, invm, curm, tmpm, mref, gref, tref, geo, MID, eig[1])
    restrict(resm, tmpm, low, mref, tref, geo, NM, NC, UP_C, "rz4", buf)

    mid = geo.nz // 2
    z_lo = mref[MASK_Z_LO : MASK_Z_LO + 1, :] > 0.5
    y_lo = mref[MASK_Y_LO : MASK_Y_LO + 1, :]
    top = mref[TOP_ROW : TOP_ROW + 1, :]

    def node(zb, a, b, c):
        return wide_load(low, zb, pl.ds((a * NC + b) * SUB + c, 1), geo)

    grid = [
        [
            node(mid, a, b, 0)
            + jnp.where(
                z_lo, roll(node(mid, a, b, 1), 1), roll(node(mid - 1, a, b, 1), -(geo.cz - 1))
            )
            for b in range(NC)
        ]
        for a in range(NC)
    ]
    xs = geo.wy * geo.cz
    floor = [grid[a][0] + y_lo * roll(grid[a][1], geo.cz) for a in range(NC)]
    base = floor[0] + roll(floor[1], xs)
    ceil = top * (grid[0][1] + roll(grid[1][1], xs))
    which = mref[DEV_ID : DEV_ID + 1, :]
    lane_dev = jnp.broadcast_to(which, (geo.planes, geo.lanes))
    row_dev = lax.broadcasted_iota(jnp.int32, (geo.planes, geo.lanes), 0).astype(jnp.float32)
    mine = lane_dev == row_dev
    owned = jnp.concatenate(
        [jnp.where(mine, base, 0.0), jnp.where(mine, ceil, 0.0)], axis=1
    )
    for k in range(nblk):
        send[:, pl.ds(k * LANES, LANES)] = dot3(owned, xhi[k], xlo[k], ((1,), (0,)))
    for pos, (ix, iy) in enumerate(devices):
        send[pl.ds(pos, 1), pl.ds(nblk * LANES, LANES)] = piece(
            ix, iy, start + nblk * slots, SUB
        )[0:1]


def coarse_kernel(*refs, geo, nblk, peers):
    parts = refs[:peers]
    xhi, xlo, mref, out = refs[peers:]
    own_ids = parts[0][:, pl.ds(nblk * LANES, LANES)]
    id_rows = jnp.concatenate([own_ids[:, k : k + 1] for k in range(nblk)], axis=0)
    picked = None
    per_step = nblk if nblk * peers * geo.planes <= 1024 else 1
    for k0 in range(0, nblk, per_step):
        ks = range(k0, k0 + per_step)
        values = jnp.concatenate(
            [parts[p][:, pl.ds(k * LANES, LANES)] for k in ks for p in range(peers)], axis=0
        )
        cols = jnp.concatenate(
            [parts[p][:, pl.ds(nblk * LANES, LANES)][:, k : k + 1] for k in ks for p in range(peers)],
            axis=0,
        )
        id_lanes = jnp.broadcast_to(cols, (cols.shape[0], LANES)).T[0:1]
        hit = (id_rows == id_lanes).astype(jnp.bfloat16)
        high, rest = split(values)
        part = dot(hit, high, ((1,), (0,))) + dot(hit, rest, ((1,), (0,)))
        picked = part if picked is None else picked + part
    full = None
    for k in range(nblk):
        part = dot3(
            picked[k * geo.planes : (k + 1) * geo.planes], xhi[k], xlo[k], ((1,), (1,))
        )
        full = part if full is None else full + part
    which = mref[DEV_ID : DEV_ID + 1, :]
    lane_dev = jnp.broadcast_to(which, (geo.planes, geo.lanes))
    row_dev = lax.broadcasted_iota(jnp.int32, (geo.planes, geo.lanes), 0).astype(jnp.float32)
    mine = lane_dev == row_dev
    for pos in range(2):
        value = full[:, pos * geo.lanes : (pos + 1) * geo.lanes]
        out[pl.ds(pos, 1), :] = jnp.sum(
            jnp.where(mine, value, 0.0), axis=0, keepdims=True
        )


def up_kernel(*refs, geo):
    solved = refs[: geo.nz]
    res, inv, cur_in, resm, invm, curm_in, gref, eig, mref, tref = refs[geo.nz : geo.nz + 10]
    out, cur, curm, tmp, tmpm, step, stepm, low, turned = refs[geo.nz + 10 :]
    y_hi = mref[MASK_Y_HI : MASK_Y_HI + 1, :] > 0.5
    z_hi = mref[MASK_Z_HI : MASK_Z_HI + 1, :] > 0.5
    xs = geo.wy * geo.cz
    levels = []
    for zb in range(geo.nz):
        base = solved[zb][0:1, :]
        ceil = solved[zb][1:2, :]
        upper = jnp.where(y_hi, roll(base, -geo.cz), ceil)
        flat = [base, upper]
        levels.append([flat, [roll(v, -xs) for v in flat]])
    for zb in range(geo.nz):
        for a in range(NC):
            for b in range(NC):
                here = levels[zb][a][b]
                after = levels[(zb + 1) % geo.nz][a][b]
                row = (a * NC + b) * SUB
                wide_store(low, zb, pl.ds(row, 1), geo, here)
                deep = jnp.where(z_hi, roll(here, -1), roll(after, geo.cz - 1))
                wide_store(low, zb, pl.ds(row + 1, 1), geo, deep)

    def copy_mid(zb, ch, row):
        curm[zb, ch, row, :] = curm_in[zb, ch, row, :]

    def copy_fine(zb, ch, row):
        cur[zb, ch, row, :] = cur_in[zb, ch, row, :]

    each_row(geo, NM, copy_mid)
    each_row(geo, NF, copy_fine)
    prolong_add(low, curm, tref, geo, NM, NC, UP_C, "pz4")
    next_smooth(resm, invm, curm, stepm, tmpm, mref, gref, tref, geo, MID, eig[1])
    prolong_add(curm, cur, tref, geo, NF, NM, UP_F, "pz8")
    next_smooth(res, inv, cur, step, tmp, mref, gref, tref, geo, FINE, eig[0])
    words = NF**3 // LANES
    mid = geo.nz // 2
    for ch in range(geo.chunks):
        for blk in range(words):
            turned[pl.ds(ch * LANES, LANES), pl.ds(blk * LANES, LANES)] = cur[
                mid, ch, pl.ds(blk * LANES, LANES), :
            ].T
    my = lax.axis_index("gx") * geo.gy + lax.axis_index("gy")
    out[...] = turned[pl.ds(pl.multiple_of(my * geo.ne, SUB), geo.ne), :]


def on_device(residual_in, geometry, eig_top, coarse_rows, block_ids, sizes):
    gx, gy, gz = sizes
    cx, cy, cz = residual_in.shape[:3]
    nblk = coarse_rows.shape[3]
    geo = Geo(gx, gy, cy, cz, 3)
    ok = cx == 1 and cz % SUB == 0 and LANES % geo.ne == 0 and geo.lanes % LANES == 0
    if not ok or coarse_rows.shape[4] != LANES or geo.planes % SUB:
        raise ValueError("block shape")
    f32 = jnp.float32
    words = NF**3 // LANES
    nodal = residual_in.reshape(geo.ne, words, LANES).transpose(1, 0, 2)
    factors = jnp.pad(geometry.reshape(3, geo.ne), ((0, SUB - 3), (0, LANES - geo.ne)))
    block = jnp.concatenate([nodal.reshape(words * geo.ne, LANES), factors], axis=0)
    prow = block.shape[0]
    ring = [(i, (i + 1) % gz) for i in range(gz)]
    back = [((i + 1) % gz, i) for i in range(gz)]
    before = lax.ppermute(block, "gz", ring)
    after = lax.ppermute(block, "gz", back)
    slots = (cy + 1) * cz
    factor = coarse_rows.reshape(slots, nblk, LANES).transpose(1, 0, 2)
    labels = jnp.pad(
        block_ids.reshape(1, nblk).astype(f32), ((0, SUB - 1), (0, LANES - nblk))
    )
    column = jnp.concatenate(
        [before, block, after, factor.reshape(nblk * slots, LANES), labels], axis=0
    )
    half, cores = geo.half, geo.cores

    def rank(ix, ih, core):
        return (ix % gx) * gy + (ih % half) * cores + core

    plane = [column]
    for dx in range(gx):
        for dh in range(half):
            if dx or dh:
                pairs = [
                    (rank(ix + dx, ih + dh, core), rank(ix, ih, core))
                    for ix in range(gx)
                    for ih in range(half)
                    for core in range(cores)
                ]
                plane.append(lax.ppermute(column, ("gx", "gy"), pairs))
    own = jnp.stack(plane)
    par = own
    if cores == 2:
        par = lax.ppermute(own, "gy", [(i, i ^ 1) for i in range(gy)])

    masks = jnp.asarray(geo.masks())
    table = jnp.asarray(TABLE)
    vmem = pl.BlockSpec(memory_space=pltpu.VMEM)
    smem = pl.BlockSpec(memory_space=pltpu.SMEM)
    fine = (geo.nz, geo.chunks, NF * NF * SUB, LANES)
    middle = (geo.nz, geo.chunks, NM * NM * SUB, LANES)
    lowest = (geo.nz, geo.chunks, NC * NC * SUB, LANES)
    wide = (nblk, 2 * geo.lanes, LANES)
    params = pltpu.CompilerParams(vmem_limit_bytes=60 * 1024 * 1024)

    def shape(dims, kind=f32):
        return jax.ShapeDtypeStruct(dims, kind)

    res, inv, cur, resm, invm, curm, gfac, xhi, xlo, send = pl.pallas_call(
        functools.partial(down_kernel, geo=geo, nblk=nblk, prow=prow),
        out_shape=[
            shape(fine),
            shape(fine),
            shape(fine),
            shape(middle),
            shape(middle),
            shape(middle),
            shape((geo.nz, geo.chunks, SUB, LANES)),
            shape(wide, jnp.bfloat16),
            shape(wide, jnp.bfloat16),
            shape((geo.planes, (nblk + 1) * LANES)),
        ],
        in_specs=[vmem, vmem, smem, vmem, vmem],
        out_specs=[vmem] * 10,
        scratch_shapes=[
            pltpu.VMEM(fine, f32),
            pltpu.VMEM(middle, f32),
            pltpu.VMEM(lowest, f32),
            pltpu.VMEM((1, 1, NM * NM * SUB, LANES), f32),
        ],
        compiler_params=params,
        name="down",
    )(own, par, eig_top, masks, table)

    parts = [send]
    for d in range(1, gz):
        parts.append(lax.ppermute(send, "gz", [((i + d) % gz, i) for i in range(gz)]))
    solved = pl.pallas_call(
        functools.partial(coarse_kernel, geo=geo, nblk=nblk, peers=gz),
        out_shape=shape((SUB, geo.lanes)),
        in_specs=[vmem] * (gz + 3),
        out_specs=vmem,
        compiler_params=params,
        name="coarse",
    )(*parts, xhi, xlo, masks)

    solved_before = lax.ppermute(solved, "gz", ring)
    solved_after = lax.ppermute(solved, "gz", back)
    out = pl.pallas_call(
        functools.partial(up_kernel, geo=geo),
        out_shape=shape((geo.ne, NF**3)),
        in_specs=[vmem] * (geo.nz + 7) + [smem, vmem, vmem],
        out_specs=vmem,
        scratch_shapes=[
            pltpu.VMEM(fine, f32),
            pltpu.VMEM(middle, f32),
            pltpu.VMEM(fine, f32),
            pltpu.VMEM(middle, f32),
            pltpu.VMEM(fine, f32),
            pltpu.VMEM(middle, f32),
            pltpu.VMEM(lowest, f32),
            pltpu.VMEM((geo.lanes, NF**3), f32),
        ],
        compiler_params=params,
        name="up",
    )(
        solved_before, solved, solved_after,
        res, inv, cur, resm, invm, curm, gfac, eig_top, masks, table,
    )
    return out.reshape(cx, cy, cz, NF**3)


def solution(mesh):
    sizes = tuple(mesh.shape[name] for name in ("gx", "gy", "gz"))
    in_specs = (
        P("gx", "gy", "gz", None),
        P(None, "gx", "gy", "gz"),
        P(),
        P("gx", "gy", "gz", None, None),
        P("gx", "gy", "gz", None),
    )
    out_specs = P("gx", "gy", "gz", None)
    return jax.shard_map(
        functools.partial(on_device, sizes=sizes),
        mesh=mesh,
        in_specs=in_specs,
        out_specs=out_specs,
        check_vma=False,
    )
```

```python
import functools
import math

import jax
import jax.numpy as jnp
import numpy as np
from jax import lax
from jax.experimental import pallas as pl
from jax.experimental.pallas import tpu as pltpu
from jax.sharding import PartitionSpec as P

NF = 8
NM = 4
NC = 2
LANES = 128
SUB = 8
SIGMA = 0.55 / 0.45
RHO0 = 1.0 / SIGMA
RHO1 = 1.0 / (2.0 * SIGMA - RHO0)


def legendre_pair(point, degree):
    previous = 1.0
    current = point
    for order in range(1, degree):
        following = ((2 * order + 1) * point * current - order * previous) / (order + 1)
        previous = current
        current = following
    return (current, previous)


def gll_tables(points):
    degree = points - 1
    node_list = []
    for index in range(points):
        guess = -math.cos(math.pi * index / degree)
        for sweep in range(100):
            high_val, low_val = legendre_pair(guess, degree)
            guess = guess - (guess * high_val - low_val) / (points * high_val)
        node_list.append(guess)
    node_list[0] = -1.0
    node_list[degree] = 1.0
    node_pos = np.array(node_list)
    at_nodes = np.array([legendre_pair(value, degree)[0] for value in node_list])
    weights = 2.0 / (degree * (degree + 1) * at_nodes**2)
    derivative = np.zeros((points, points))
    for row_pos in range(points):
        for col_pos in range(points):
            if row_pos != col_pos:
                derivative[row_pos, col_pos] = at_nodes[row_pos] / (
                    at_nodes[col_pos] * (node_pos[row_pos] - node_pos[col_pos])
                )
    derivative[0, 0] = -degree * (degree + 1) / 4.0
    derivative[degree, degree] = degree * (degree + 1) / 4.0
    stiffness = derivative.T @ (weights[:, None] * derivative)
    return (node_pos, weights, stiffness)


def interp_table(fine_pts, coarse_pts):
    fine_nodes = gll_tables(fine_pts)[0]
    coarse_nodes = gll_tables(coarse_pts)[0]
    lagrange = np.ones((fine_pts, coarse_pts))
    for col_pos in range(coarse_pts):
        for other_pos in range(coarse_pts):
            if other_pos != col_pos:
                lagrange[:, col_pos] *= (fine_nodes - coarse_nodes[other_pos]) / (
                    coarse_nodes[col_pos] - coarse_nodes[other_pos]
                )
    return lagrange


class Level:
    def __init__(self, points):
        self.n = points
        _, weights, stiffness = gll_tables(points)
        self.w = [float(v) for v in weights]
        self.kd = [float(v) for v in np.diag(stiffness)]
        scaled = stiffness / weights[:, None]
        half = points // 2
        flipped = scaled[:, ::-1]
        self.even = [[float(v) for v in row[:half]] for row in (scaled + flipped)[:half] / 2]
        self.odd = [[float(v) for v in row[:half]] for row in (scaled - flipped)[:half] / 2]
        self.scaled = scaled
        self.weights = weights
        self.diag = np.diag(stiffness)


FINE = Level(NF)
MID = Level(NM)
UP_F = interp_table(NF, NM)
UP_C = interp_table(NM, NC)


def shared_faces(lagrange):
    out = lagrange.copy()
    out[0] *= 0.5
    out[-1] *= 0.5
    return out


def pad_rows(column, fill=0.0):
    out = np.full((SUB,), fill)
    out[: column.shape[0]] = column
    return out


def build_tables():
    rows = []
    index = {}

    def put(name, columns):
        index[name] = len(rows)
        rows.extend(columns)

    put("kz8", [FINE.scaled[:, c] for c in range(NF)])
    put("kz4", [pad_rows(MID.scaled[:, c]) for c in range(NM)])
    put("w8", [FINE.weights])
    put("w4", [pad_rows(MID.weights, 1.0)])
    put("kd8", [FINE.diag])
    put("kd4", [pad_rows(MID.diag, 1.0)])
    put("rz8", [pad_rows(shared_faces(UP_F)[c]) for c in range(NF)])
    put("rz4", [pad_rows(shared_faces(UP_C)[c]) for c in range(NM)])
    put("pz8", [UP_F[:, c] for c in range(NM)])
    put("pz4", [pad_rows(UP_C[:, c]) for c in range(NC)])
    flat = np.concatenate(rows).astype(np.float32)
    return np.ascontiguousarray(np.broadcast_to(flat[:, None], (flat.shape[0], LANES))), index


TABLE, TINDEX = build_tables()
MASK_Y_LO, MASK_Y_HI, MASK_Z_LO, MASK_Z_HI, FAC_Y_LO, FAC_Y_HI, DEV_ID, TOP_ROW = range(8)


class Geo:
    def __init__(self, gx, gy, cy, cz, nz):
        self.gx, self.gy, self.cy, self.cz, self.nz = gx, gy, cy, cz, nz
        self.wy = gy * cy
        self.lanes = gx * self.wy * cz
        self.ne = cy * cz
        self.planes = gx * gy
        self.half = gy // 2 if gy % 2 == 0 else gy
        self.cores = gy // self.half
        self.chunks = self.lanes // LANES

    def masks(self):
        lane = np.arange(self.lanes)
        z = lane % self.cz
        y = (lane // self.cz) % self.wy
        out = np.zeros((8, self.lanes), np.float32)
        out[MASK_Y_LO] = y > 0
        out[MASK_Y_HI] = y < self.wy - 1
        out[MASK_Z_LO] = z > 0
        out[MASK_Z_HI] = z < self.cz - 1
        out[FAC_Y_LO] = np.where(y > 0, 0.5, 1.0)
        out[FAC_Y_HI] = np.where(y < self.wy - 1, 0.5, 1.0)
        out[DEV_ID] = lane // self.ne
        out[TOP_ROW] = y == self.wy - 1
        return out


def roll(value, shift):
    size = value.shape[-1]
    shift %= size
    return value if shift == 0 else pltpu.roll(value, shift, axis=value.ndim - 1)


def tab(tref, name, pos=0):
    return tref[pl.ds((TINDEX[name] + pos) * SUB, SUB), :]


def lane_ds(chunk):
    if isinstance(chunk, int):
        return pl.ds(chunk * LANES, LANES)
    return pl.ds(pl.multiple_of(chunk * LANES, LANES), LANES)


def for_tiles(geo, body):
    def step(pos, carry):
        if geo.chunks == 1:
            body(pos, 0)
        else:
            body(pos // geo.chunks, pos % geo.chunks)
        return carry

    lax.fori_loop(0, geo.nz * geo.chunks, step, 0)


def loop(count, body):
    def step(pos, carry):
        body(pos)
        return carry

    lax.fori_loop(0, count, step, 0)


def rows8(pos):
    if isinstance(pos, int):
        return pl.ds(pos * SUB, SUB)
    return pl.ds(pl.multiple_of(pos * SUB, SUB), SUB)


def wide_load(ref, zb, rows, geo):
    parts = [ref[zb, ch, rows, :] for ch in range(geo.chunks)]
    return parts[0] if len(parts) == 1 else jnp.concatenate(parts, axis=1)


def wide_store(ref, zb, rows, geo, value):
    for ch in range(geo.chunks):
        ref[zb, ch, rows, :] = value[:, ch * LANES : (ch + 1) * LANES]


def gather_sum(ref, mref, geo, n):
    xs = geo.wy * geo.cz
    last = (n - 1) * n
    for b in range(n):
        for zb in range(geo.nz):
            low = wide_load(ref, zb, rows8(b), geo)
            high = wide_load(ref, zb, rows8(last + b), geo)
            wide_store(ref, zb, rows8(b), geo, low + roll(high, xs))
            wide_store(ref, zb, rows8(last + b), geo, high + roll(low, -xs))
    y_lo = mref[MASK_Y_LO : MASK_Y_LO + 1, :]
    y_hi = mref[MASK_Y_HI : MASK_Y_HI + 1, :]
    for a in range(n):
        first, final = rows8(a * n), rows8(a * n + n - 1)
        for zb in range(geo.nz):
            low = wide_load(ref, zb, first, geo)
            high = wide_load(ref, zb, final, geo)
            wide_store(ref, zb, first, geo, low + y_lo * roll(high, geo.cz))
            wide_store(ref, zb, final, geo, high + y_hi * roll(low, -geo.cz))
    z_lo = mref[MASK_Z_LO : MASK_Z_LO + 1, :] > 0.5
    z_hi = mref[MASK_Z_HI : MASK_Z_HI + 1, :] > 0.5
    group = min(SUB, n * n)
    for g in range(n * n // group):
        first = pl.ds(g * group * SUB, group, stride=SUB)
        final = pl.ds(g * group * SUB + n - 1, group, stride=SUB)
        low = [wide_load(ref, zb, first, geo) for zb in range(geo.nz)]
        high = [wide_load(ref, zb, final, geo) for zb in range(geo.nz)]
        for zb in range(geo.nz):
            before = roll(high[(zb - 1) % geo.nz], -(geo.cz - 1))
            after = roll(low[(zb + 1) % geo.nz], geo.cz - 1)
            near = jnp.where(z_lo, roll(high[zb], 1), before)
            wide_store(ref, zb, first, geo, low[zb] + near)
            near = jnp.where(z_hi, roll(low[zb], -1), after)
            wide_store(ref, zb, final, geo, high[zb] + near)


def contract(values, level):
    half = level.n // 2
    sums = [values[a] + values[level.n - 1 - a] for a in range(half)]
    diffs = [values[a] - values[level.n - 1 - a] for a in range(half)]
    out = [None] * level.n
    for i in range(half):
        even = sums[0] * level.even[i][0]
        odd = diffs[0] * level.odd[i][0]
        for a in range(1, half):
            even = even + sums[a] * level.even[i][a]
            odd = odd + diffs[a] * level.odd[i][a]
        out[i] = even + odd
        out[level.n - 1 - i] = even - odd
    return out


def combine(values, table):
    out = []
    for i in range(table.shape[0]):
        total = values[0] * float(table[i, 0])
        for a in range(1, table.shape[1]):
            total = total + values[a] * float(table[i, a])
        out.append(total)
    return out


def sublane_mix(ref, zb, ch, row, columns):
    total = ref[zb, ch, pl.ds(row, 1), :] * columns[0]
    for c in range(1, len(columns)):
        total = total + ref[zb, ch, pl.ds(row + c, 1), :] * columns[c]
    return total


def apply_local(src, dst, gref, tref, geo, level):
    n = level.n
    kname, wname = ("kz8", "w8") if n == NF else ("kz4", "w4")

    def body(zb, ch):
        ln = lane_ds(ch)
        wc = tab(tref, wname)
        gw = [gref[zb, ch, pl.ds(i, 1), :] * wc for i in range(3)]
        columns = [tab(tref, kname, c) for c in range(n)]
        for b in range(n):
            mixed = contract([src[zb, ch, rows8(a * n + b), :] for a in range(n)], level)
            for a in range(n):
                dst[zb, ch, rows8(a * n + b), :] = mixed[a] * gw[0]
        for a in range(n):
            mixed = contract([src[zb, ch, rows8(a * n + b), :] for b in range(n)], level)
            for b in range(n):
                row = (a * n + b) * SUB
                along = sublane_mix(src, zb, ch, row, columns)
                total = dst[zb, ch, rows8(a * n + b), :] + mixed[b] * gw[1] + along * gw[2]
                dst[zb, ch, rows8(a * n + b), :] = total * (level.w[a] * level.w[b])

    for_tiles(geo, body)


def local_diagonal(dst, gref, tref, geo, level):
    n = level.n
    wname, dname = ("w8", "kd8") if n == NF else ("w4", "kd4")

    def body(zb, ch):
        ln = lane_ds(ch)
        wc = tab(tref, wname)
        gx = gref[zb, ch, pl.ds(0, 1), :] * wc
        gy = gref[zb, ch, pl.ds(1, 1), :] * wc
        gz = gref[zb, ch, pl.ds(2, 1), :] * tab(tref, dname)
        for a in range(n):
            for b in range(n):
                dst[zb, ch, rows8(a * n + b), :] = (
                    gx * (level.kd[a] * level.w[b])
                    + gy * (level.w[a] * level.kd[b])
                    + gz * (level.w[a] * level.w[b])
                )

    for_tiles(geo, body)


def each_row(geo, n, body):
    def tile(zb, ch):
        for row in range(n * n):
            body(zb, ch, rows8(row))

    for_tiles(geo, tile)


def first_smooth(res, inv, cur, tmp, mref, gref, tref, geo, level, top):
    first = 1.0 / (0.55 * top)
    second = 2.0 * RHO1 / (0.45 * top)

    def start(zb, ch, row):
        value = 1.0 / tmp[zb, ch, row, :]
        inv[zb, ch, row, :] = value
        cur[zb, ch, row, :] = value * res[zb, ch, row, :] * first

    each_row(geo, level.n, start)
    apply_local(cur, tmp, gref, tref, geo, level)
    gather_sum(tmp, mref, geo, level.n)

    def finish(zb, ch, row):
        left = res[zb, ch, row, :] - tmp[zb, ch, row, :]
        cur[zb, ch, row, :] = (1.0 + RHO0 * RHO1) * cur[zb, ch, row, :] + second * (
            inv[zb, ch, row, :] * left
        )

    each_row(geo, level.n, finish)
    apply_local(cur, tmp, gref, tref, geo, level)
    gather_sum(tmp, mref, geo, level.n)


def next_smooth(res, inv, cur, step, tmp, mref, gref, tref, geo, level, top):
    first = 1.0 / (0.55 * top)
    second = 2.0 * RHO1 / (0.45 * top)
    apply_local(cur, tmp, gref, tref, geo, level)
    gather_sum(tmp, mref, geo, level.n)

    def start(zb, ch, row):
        value = inv[zb, ch, row, :] * (res[zb, ch, row, :] - tmp[zb, ch, row, :]) * first
        step[zb, ch, row, :] = value
        cur[zb, ch, row, :] = cur[zb, ch, row, :] + value

    each_row(geo, level.n, start)
    apply_local(cur, tmp, gref, tref, geo, level)
    gather_sum(tmp, mref, geo, level.n)

    def finish(zb, ch, row):
        left = res[zb, ch, row, :] - tmp[zb, ch, row, :]
        cur[zb, ch, row, :] = (
            cur[zb, ch, row, :]
            + (RHO0 * RHO1) * step[zb, ch, row, :]
            + second * (inv[zb, ch, row, :] * left)
        )

    each_row(geo, level.n, finish)


def restrict(res, tmp, dst, mref, tref, geo, nf, nc, table, name, buf):
    scaled = shared_faces(table)

    def body(zb, ch):
        ln = lane_ds(ch)
        f_lo = mref[FAC_Y_LO : FAC_Y_LO + 1, ln]
        f_hi = mref[FAC_Y_HI : FAC_Y_HI + 1, ln]
        part = []
        for b in range(nf):
            values = []
            for a in range(nf):
                row = rows8(a * nf + b)
                values.append(res[zb, ch, row, :] - tmp[zb, ch, row, :])
            mixed = combine(values, scaled.T)
            if b == 0:
                mixed = [v * f_lo for v in mixed]
            if b == nf - 1:
                mixed = [v * f_hi for v in mixed]
            part.append(mixed)
        columns = [tab(tref, name, c) for c in range(nf)]
        for i in range(nc):
            along = combine([part[b][i] for b in range(nf)], table.T)
            for j in range(nc):
                buf[0, 0, rows8(i * nc + j), :] = along[j]
        for row in range(nc * nc):
            dst[zb, ch, rows8(row), :] = sublane_mix(buf, 0, 0, row * SUB, columns)

    for_tiles(geo, body)


def prolong_add(src, cur, tref, geo, nf, nc, table, name):
    def body(zb, ch):
        ln = lane_ds(ch)
        columns = [tab(tref, name, c) for c in range(nc)]
        part = []
        for a in range(nc):
            deep = [
                sublane_mix(src, zb, ch, (a * nc + b) * SUB, columns) for b in range(nc)
            ]
            part.append(combine(deep, table))
        for b in range(nf):
            mixed = combine([part[a][b] for a in range(nc)], table)
            for a in range(nf):
                row = rows8(a * nf + b)
                cur[zb, ch, row, :] = cur[zb, ch, row, :] + mixed[a]

    for_tiles(geo, body)


def split(value):
    high = value.astype(jnp.bfloat16)
    return high, (value - high.astype(jnp.float32)).astype(jnp.bfloat16)


def dot(left, right, dims):
    return lax.dot_general(left, right, (dims, ((), ())), preferred_element_type=jnp.float32)


def dot3(left, right_high, right_low, dims):
    high, low = split(left)
    return dot(high, right_high, dims) + (dot(high, right_low, dims) + dot(low, right_high, dims))


def pieces_of(own, par, geo):
    my_x = lax.axis_index("gx")
    my_y = lax.axis_index("gy")
    my_h = my_y // geo.cores
    my_c = my_y % geo.cores

    def piece(ix, iy, start, size):
        rel = lax.rem(ix - my_x + geo.gx, geo.gx) * geo.half + lax.rem(
            iy // geo.cores - my_h + geo.half, geo.half
        )
        mine = own[rel, pl.ds(start, size), :]
        if geo.cores == 1:
            return mine
        return jnp.where(my_c == iy % geo.cores, mine, par[rel, pl.ds(start, size), :])

    return piece


def pack_kernel(residual, geometry, out, *, geo):
    words = NF**3 // LANES
    for blk in range(words):
        out[pl.ds(blk * geo.ne, geo.ne), :] = residual[:, pl.ds(blk * LANES, LANES)]
    factors = [geometry[:, 0, y, :] for y in range(geo.cy)]
    factors.append(jnp.zeros((3, LANES - geo.ne), jnp.float32))
    out[pl.ds(words * geo.ne, SUB), :] = jnp.concatenate(
        [jnp.concatenate(factors, axis=1), jnp.zeros((SUB - 3, LANES), jnp.float32)], axis=0
    )


def factor_kernel(own, par, xhi, xlo, labels, *, geo, nblk):
    piece = pieces_of(own, par, geo)
    devices = [(ix, iy) for ix in range(geo.gx) for iy in range(geo.gy)]

    def start(slot, k):
        return (slot * nblk + k) * geo.cz

    for k in range(nblk):
        rows = [
            piece(ix, iy, start(slot, k), geo.cz) for ix, iy in devices for slot in range(geo.cy)
        ]
        for ix in range(geo.gx):
            rows.append(jnp.zeros(((geo.wy - 1) * geo.cz, LANES), jnp.float32))
            rows.append(piece(ix, geo.gy - 1, start(geo.cy, k), geo.cz))
        high, rest = split(jnp.concatenate(rows, axis=0))
        xhi[k] = high
        xlo[k] = rest
    for pos, (ix, iy) in enumerate(devices):
        labels[pl.ds(pos, 1), :] = piece(ix, iy, start(geo.cy + 1, 0), SUB)[0:1]


def down_kernel(own, par, eig, mref, tref, xhi, xlo, labels, *refs, geo, nblk, prow):
    res, inv, cur, resm, invm, curm, gref, send, tmp, tmpm, low, buf = refs
    piece = pieces_of(own, par, geo)
    devices = [(ix, iy) for ix in range(geo.gx) for iy in range(geo.gy)]
    per_chunk = LANES // geo.ne
    words = NF**3 // LANES
    for zb in range(geo.nz):
        for ch in range(geo.chunks):
            group = devices[ch * per_chunk : (ch + 1) * per_chunk]
            for blk in range(words):
                rows = [piece(ix, iy, zb * prow + blk * geo.ne, geo.ne) for ix, iy in group]
                square = jnp.concatenate(rows, axis=0)
                res[zb, ch, pl.ds(blk * LANES, LANES), :] = square.T
            total = None
            for pos, (ix, iy) in enumerate(group):
                part = roll(piece(ix, iy, zb * prow + words * geo.ne, SUB), pos * geo.ne)
                total = part if total is None else total + part
            gref[zb, ch] = total
    gather_sum(res, mref, geo, NF)
    local_diagonal(tmp, gref, tref, geo, FINE)
    gather_sum(tmp, mref, geo, NF)
    first_smooth(res, inv, cur, tmp, mref, gref, tref, geo, FINE, eig[0])
    restrict(res, tmp, resm, mref, tref, geo, NF, NM, UP_F, "rz8", buf)
    gather_sum(resm, mref, geo, NM)
    local_diagonal(tmpm, gref, tref, geo, MID)
    gather_sum(tmpm, mref, geo, NM)
    first_smooth(resm, invm, curm, tmpm, mref, gref, tref, geo, MID, eig[1])
    restrict(resm, tmpm, low, mref, tref, geo, NM, NC, UP_C, "rz4", buf)

    mid = geo.nz // 2
    z_lo = mref[MASK_Z_LO : MASK_Z_LO + 1, :] > 0.5
    y_lo = mref[MASK_Y_LO : MASK_Y_LO + 1, :]
    top = mref[TOP_ROW : TOP_ROW + 1, :]

    def node(zb, a, b, c):
        return wide_load(low, zb, pl.ds((a * NC + b) * SUB + c, 1), geo)

    grid = [
        [
            node(mid, a, b, 0)
            + jnp.where(
                z_lo, roll(node(mid, a, b, 1), 1), roll(node(mid - 1, a, b, 1), -(geo.cz - 1))
            )
            for b in range(NC)
        ]
        for a in range(NC)
    ]
    xs = geo.wy * geo.cz
    floor = [grid[a][0] + y_lo * roll(grid[a][1], geo.cz) for a in range(NC)]
    base = floor[0] + roll(floor[1], xs)
    ceil = top * (grid[0][1] + roll(grid[1][1], xs))
    which = mref[DEV_ID : DEV_ID + 1, :]
    lane_dev = jnp.broadcast_to(which, (geo.planes, geo.lanes))
    row_dev = lax.broadcasted_iota(jnp.int32, (geo.planes, geo.lanes), 0).astype(jnp.float32)
    mine = lane_dev == row_dev
    owned = jnp.concatenate(
        [jnp.where(mine, base, 0.0), jnp.where(mine, ceil, 0.0)], axis=1
    )
    for k in range(nblk):
        send[:, pl.ds(k * LANES, LANES)] = dot3(owned, xhi[k], xlo[k], ((1,), (0,)))
    send[:, pl.ds(nblk * LANES, LANES)] = labels[...]


def coarse_kernel(*refs, geo, nblk, peers):
    parts = refs[:peers]
    xhi, xlo, mref, out = refs[peers:]
    own_ids = parts[0][:, pl.ds(nblk * LANES, LANES)]
    id_rows = jnp.concatenate([own_ids[:, k : k + 1] for k in range(nblk)], axis=0)
    picked = None
    per_step = nblk if nblk * peers * geo.planes <= 1024 else 1
    for k0 in range(0, nblk, per_step):
        ks = range(k0, k0 + per_step)
        values = jnp.concatenate(
            [parts[p][:, pl.ds(k * LANES, LANES)] for k in ks for p in range(peers)], axis=0
        )
        cols = jnp.concatenate(
            [parts[p][:, pl.ds(nblk * LANES, LANES)][:, k : k + 1] for k in ks for p in range(peers)],
            axis=0,
        )
        id_lanes = jnp.broadcast_to(cols, (cols.shape[0], LANES)).T[0:1]
        hit = (id_rows == id_lanes).astype(jnp.bfloat16)
        high, rest = split(values)
        part = dot(hit, high, ((1,), (0,))) + dot(hit, rest, ((1,), (0,)))
        picked = part if picked is None else picked + part
    full = None
    for k in range(nblk):
        part = dot3(
            picked[k * geo.planes : (k + 1) * geo.planes], xhi[k], xlo[k], ((1,), (1,))
        )
        full = part if full is None else full + part
    which = mref[DEV_ID : DEV_ID + 1, :]
    lane_dev = jnp.broadcast_to(which, (geo.planes, geo.lanes))
    row_dev = lax.broadcasted_iota(jnp.int32, (geo.planes, geo.lanes), 0).astype(jnp.float32)
    mine = lane_dev == row_dev
    for pos in range(2):
        value = full[:, pos * geo.lanes : (pos + 1) * geo.lanes]
        out[pl.ds(pos, 1), :] = jnp.sum(
            jnp.where(mine, value, 0.0), axis=0, keepdims=True
        )


def up_kernel(*refs, geo):
    solved = refs[: geo.nz]
    res, inv, cur_in, resm, invm, curm_in, gref, eig, mref, tref = refs[geo.nz : geo.nz + 10]
    out, cur, curm, tmp, tmpm, step, stepm, low, turned = refs[geo.nz + 10 :]
    y_hi = mref[MASK_Y_HI : MASK_Y_HI + 1, :] > 0.5
    z_hi = mref[MASK_Z_HI : MASK_Z_HI + 1, :] > 0.5
    xs = geo.wy * geo.cz
    levels = []
    for zb in range(geo.nz):
        base = solved[zb][0:1, :]
        ceil = solved[zb][1:2, :]
        upper = jnp.where(y_hi, roll(base, -geo.cz), ceil)
        flat = [base, upper]
        levels.append([flat, [roll(v, -xs) for v in flat]])
    for zb in range(geo.nz):
        for a in range(NC):
            for b in range(NC):
                here = levels[zb][a][b]
                after = levels[(zb + 1) % geo.nz][a][b]
                row = (a * NC + b) * SUB
                wide_store(low, zb, pl.ds(row, 1), geo, here)
                deep = jnp.where(z_hi, roll(here, -1), roll(after, geo.cz - 1))
                wide_store(low, zb, pl.ds(row + 1, 1), geo, deep)

    def copy_mid(zb, ch, row):
        curm[zb, ch, row, :] = curm_in[zb, ch, row, :]

    def copy_fine(zb, ch, row):
        cur[zb, ch, row, :] = cur_in[zb, ch, row, :]

    each_row(geo, NM, copy_mid)
    each_row(geo, NF, copy_fine)
    prolong_add(low, curm, tref, geo, NM, NC, UP_C, "pz4")
    next_smooth(resm, invm, curm, stepm, tmpm, mref, gref, tref, geo, MID, eig[1])
    prolong_add(curm, cur, tref, geo, NF, NM, UP_F, "pz8")
    next_smooth(res, inv, cur, step, tmp, mref, gref, tref, geo, FINE, eig[0])
    words = NF**3 // LANES
    mid = geo.nz // 2
    for ch in range(geo.chunks):
        for blk in range(words):
            turned[pl.ds(ch * LANES, LANES), pl.ds(blk * LANES, LANES)] = cur[
                mid, ch, pl.ds(blk * LANES, LANES), :
            ].T
    my = lax.axis_index("gx") * geo.gy + lax.axis_index("gy")
    out[...] = turned[pl.ds(pl.multiple_of(my * geo.ne, SUB), geo.ne), :]


def on_device(residual_in, geometry, eig_top, coarse_rows, block_ids, sizes):
    gx, gy, gz = sizes
    cx, cy, cz = residual_in.shape[:3]
    nblk = coarse_rows.shape[3]
    geo = Geo(gx, gy, cy, cz, 3)
    ok = cx == 1 and cz % SUB == 0 and LANES % geo.ne == 0 and geo.lanes % LANES == 0
    if not ok or coarse_rows.shape[4] != LANES or geo.planes % SUB:
        raise ValueError("block shape")
    f32 = jnp.float32
    vmem = pl.BlockSpec(memory_space=pltpu.VMEM)
    smem = pl.BlockSpec(memory_space=pltpu.SMEM)
    half, cores = geo.half, geo.cores
    slots = (cy + 1) * cz
    prow = NF**3 // LANES * geo.ne + SUB

    def shape(dims, kind=f32):
        return jax.ShapeDtypeStruct(dims, kind)

    def call(body, name, specs, outs, scratch, *operands):
        kept = list(operands) + list(outs) + list(scratch)
        total = sum(math.prod(a.shape) * a.dtype.itemsize for a in kept)
        return pl.pallas_call(
            body,
            out_shape=list(outs),
            in_specs=specs,
            out_specs=[vmem] * len(outs),
            scratch_shapes=[pltpu.VMEM(a.shape, a.dtype) for a in scratch],
            compiler_params=pltpu.CompilerParams(
                vmem_limit_bytes=min(total + (3 << 20), 60 << 20)
            ),
            name=name,
        )(*operands)

    def rank(ix, ih, core):
        return (ix % gx) * gy + (ih % half) * cores + core

    def across_chips(value):
        parts = [value]
        for dx in range(gx):
            for dh in range(half):
                if dx or dh:
                    pairs = [
                        (rank(ix + dx, ih + dh, core), rank(ix, ih, core))
                        for ix in range(gx)
                        for ih in range(half)
                        for core in range(cores)
                    ]
                    parts.append(lax.ppermute(value, ("gx", "gy"), pairs))
        return jnp.stack(parts)

    def between_cores(value):
        if cores == 1:
            return value
        return lax.ppermute(value, "gy", [(i, i ^ 1) for i in range(gy)])

    (block,) = call(
        functools.partial(pack_kernel, geo=geo),
        "pack",
        [vmem, vmem],
        [shape((prow, LANES))],
        [],
        residual_in.reshape(geo.ne, NF**3),
        geometry,
    )
    ring = [(i, (i + 1) % gz) for i in range(gz)]
    back = [((i + 1) % gz, i) for i in range(gz)]
    before = lax.ppermute(block, "gz", ring)
    after = lax.ppermute(block, "gz", back)

    labels = jnp.pad(
        block_ids.reshape(1, nblk).astype(f32), ((0, SUB - 1), (0, LANES - nblk))
    )
    factor = coarse_rows.reshape(cy + 1, cz, nblk, LANES).transpose(0, 2, 1, 3)
    factor = jnp.concatenate([factor.reshape(slots * nblk, LANES), labels], axis=0)
    factor_own = across_chips(factor)
    factor_par = between_cores(factor_own)

    own = across_chips(jnp.concatenate([before, block, after], axis=0))
    par = between_cores(own)

    masks = jnp.asarray(geo.masks())
    table = jnp.asarray(TABLE)
    fine = shape((geo.nz, geo.chunks, NF * NF * SUB, LANES))
    middle = shape((geo.nz, geo.chunks, NM * NM * SUB, LANES))
    lowest = shape((geo.nz, geo.chunks, NC * NC * SUB, LANES))
    wide = shape((nblk, 2 * geo.lanes, LANES), jnp.bfloat16)

    xhi, xlo, names = call(
        functools.partial(factor_kernel, geo=geo, nblk=nblk),
        "factor",
        [vmem, vmem],
        [wide, wide, shape((geo.planes, LANES))],
        [],
        factor_own,
        factor_par,
    )
    res, inv, cur, resm, invm, curm, gfac, send = call(
        functools.partial(down_kernel, geo=geo, nblk=nblk, prow=prow),
        "down",
        [vmem, vmem, smem] + [vmem] * 5,
        [fine] * 3
        + [middle] * 3
        + [shape((geo.nz, geo.chunks, SUB, LANES)), shape((geo.planes, (nblk + 1) * LANES))],
        [fine, middle, lowest, shape((1, 1, NM * NM * SUB, LANES))],
        own, par, eig_top, masks, table, xhi, xlo, names,
    )

    parts = [send]
    for d in range(gz - 1, 0, -1):
        pairs = [((i + d) % gz, i) for i in range(gz)]
        if gz & (gz - 1) == 0:
            pairs = [(i ^ d, i) for i in range(gz)]
        parts.append(lax.ppermute(send, "gz", pairs))
    (solved,) = call(
        functools.partial(coarse_kernel, geo=geo, nblk=nblk, peers=gz),
        "coarse",
        [vmem] * (gz + 3),
        [shape((SUB, geo.lanes))],
        [],
        *parts, xhi, xlo, masks,
    )

    solved_before = lax.ppermute(solved, "gz", ring)
    solved_after = lax.ppermute(solved, "gz", back)
    (out,) = call(
        functools.partial(up_kernel, geo=geo),
        "up",
        [vmem] * (geo.nz + 7) + [smem, vmem, vmem],
        [shape((geo.ne, NF**3))],
        [fine, middle, fine, middle, fine, middle, lowest, shape((geo.lanes, NF**3))],
        solved_before, solved, solved_after,
        res, inv, cur, resm, invm, curm, gfac, eig_top, masks, table,
    )
    return out.reshape(cx, cy, cz, NF**3)


def solution(mesh):
    sizes = tuple(mesh.shape[name] for name in ("gx", "gy", "gz"))
    in_specs = (
        P("gx", "gy", "gz", None),
        P(None, "gx", "gy", "gz"),
        P(),
        P("gx", "gy", "gz", None, None),
        P("gx", "gy", "gz", None),
    )
    out_specs = P("gx", "gy", "gz", None)
    return jax.shard_map(
        functools.partial(on_device, sizes=sizes),
        mesh=mesh,
        in_specs=in_specs,
        out_specs=out_specs,
        check_vma=False,
    )
```

```python
import functools
import math

import jax
import jax.numpy as jnp
import numpy as np
from jax import lax
from jax.experimental import pallas as pl
from jax.experimental.pallas import tpu as pltpu
from jax.sharding import PartitionSpec as P


NF = 8
NM = 4
NC = 2
LANES = 128
SUB = 8
MAX_EVERYWHERE = 2 << 20
SIGMA = 0.55 / 0.45
RHO0 = 1.0 / SIGMA
RHO1 = 1.0 / (2.0 * SIGMA - RHO0)


def legendre_pair(point, degree):
    previous = 1.0
    current = point
    for order in range(1, degree):
        following = ((2 * order + 1) * point * current - order * previous) / (order + 1)
        previous = current
        current = following
    return (current, previous)


def gll_tables(points):
    degree = points - 1
    node_list = []
    for index in range(points):
        guess = -math.cos(math.pi * index / degree)
        for _ in range(100):
            high_val, low_val = legendre_pair(guess, degree)
            guess = guess - (guess * high_val - low_val) / (points * high_val)
        node_list.append(guess)
    node_list[0] = -1.0
    node_list[degree] = 1.0
    node_pos = np.array(node_list)
    at_nodes = np.array([legendre_pair(value, degree)[0] for value in node_list])
    weights = 2.0 / (degree * (degree + 1) * at_nodes**2)
    derivative = np.zeros((points, points))
    for row_pos in range(points):
        for col_pos in range(points):
            if row_pos != col_pos:
                derivative[row_pos, col_pos] = at_nodes[row_pos] / (
                    at_nodes[col_pos] * (node_pos[row_pos] - node_pos[col_pos])
                )
    derivative[0, 0] = -degree * (degree + 1) / 4.0
    derivative[degree, degree] = degree * (degree + 1) / 4.0
    stiffness = derivative.T @ (weights[:, None] * derivative)
    return (node_pos, weights, stiffness)


def interp_table(fine_pts, coarse_pts):
    fine_nodes = gll_tables(fine_pts)[0]
    coarse_nodes = gll_tables(coarse_pts)[0]
    lagrange = np.ones((fine_pts, coarse_pts))
    for col_pos in range(coarse_pts):
        for other_pos in range(coarse_pts):
            if other_pos != col_pos:
                lagrange[:, col_pos] *= (fine_nodes - coarse_nodes[other_pos]) / (
                    coarse_nodes[col_pos] - coarse_nodes[other_pos]
                )
    return lagrange


class Level:
    def __init__(self, points):
        self.n = points
        _, weights, stiffness = gll_tables(points)
        self.w = [float(v) for v in weights]
        self.kd = [float(v) for v in np.diag(stiffness)]
        scaled = stiffness / weights[:, None]
        half = points // 2
        flipped = scaled[:, ::-1]
        self.even = [[float(v) for v in row[:half]] for row in (scaled + flipped)[:half] / 2]
        self.odd = [[float(v) for v in row[:half]] for row in (scaled - flipped)[:half] / 2]
        self.scaled = scaled
        self.weights = weights
        self.diag = np.diag(stiffness)


FINE = Level(NF)
MID = Level(NM)
UP_F = interp_table(NF, NM)
UP_C = interp_table(NM, NC)


def shared_faces(lagrange):
    out = lagrange.copy()
    out[0] *= 0.5
    out[-1] *= 0.5
    return out


def pad_rows(column, fill=0.0):
    out = np.full((SUB,), fill)
    out[: column.shape[0]] = column
    return out


def build_tables():
    rows = []
    index = {}

    def put(name, columns):
        index[name] = len(rows)
        rows.extend(columns)

    put("kz8", [FINE.scaled[:, c] for c in range(NF)])
    put("kz4", [pad_rows(MID.scaled[:, c]) for c in range(NM)])
    put("w8", [FINE.weights])
    put("w4", [pad_rows(MID.weights, 1.0)])
    put("kd8", [FINE.diag])
    put("kd4", [pad_rows(MID.diag, 1.0)])
    put("rz8", [pad_rows(shared_faces(UP_F)[c]) for c in range(NF)])
    put("rz4", [pad_rows(shared_faces(UP_C)[c]) for c in range(NM)])
    put("pz8", [UP_F[:, c] for c in range(NM)])
    put("pz4", [pad_rows(UP_C[:, c]) for c in range(NC)])
    flat = np.concatenate(rows).astype(np.float32)
    return np.ascontiguousarray(np.broadcast_to(flat[:, None], (flat.shape[0], LANES))), index


TABLE, TINDEX = build_tables()
MASK_Y_LO, MASK_Y_HI, MASK_Z_LO, MASK_Z_HI, FAC_Y_LO, FAC_Y_HI, TOP_ROW, NEXT_Z = range(8)


class Geo:
    def __init__(self, gx, gy, cy, cz, nz):
        self.gx, self.gy, self.cy, self.cz, self.nz = gx, gy, cy, cz, nz
        self.wy = gy * cy
        self.lanes = gx * self.wy * cz
        self.ne = cy * cz
        self.planes = gx * gy
        self.half = gy // 2 if gy % 2 == 0 else gy
        self.cores = gy // self.half
        self.chunks = self.lanes // LANES
        self.mid = 1

    def window(self, nz, mid=1):
        out = Geo(self.gx, self.gy, self.cy, self.cz, nz)
        out.mid = mid
        return out

    def owners(self, everywhere):
        lane = np.arange(self.lanes)
        y = (lane // self.cz) % self.wy
        x = lane // (self.cz * self.wy)
        last = x * self.gy + self.gy - 1
        if everywhere:
            parts = [zb * self.planes + lane // self.ne for zb in range(self.nz)]
            zb = self.wy - 1 - y
            parts.append(np.where(zb < self.nz, zb * self.planes + last, -1))
        else:
            parts = [lane // self.ne, np.where(y == self.wy - 1, last, -1)]
        return np.tile(np.concatenate(parts).astype(np.float32), (SUB, 1))

    def masks(self):
        lane = np.arange(self.lanes)
        z = lane % self.cz
        y = (lane // self.cz) % self.wy
        out = np.zeros((8, self.lanes), np.float32)
        out[MASK_Y_LO] = y > 0
        out[MASK_Y_HI] = y < self.wy - 1
        out[MASK_Z_LO] = z > 0
        out[MASK_Z_HI] = z < self.cz - 1
        out[FAC_Y_LO] = np.where(y > 0, 0.5, 1.0)
        out[FAC_Y_HI] = np.where(y < self.wy - 1, 0.5, 1.0)
        out[TOP_ROW] = y == self.wy - 1
        out[NEXT_Z] = z < self.cz // 2
        return out


def roll(value, shift):
    size = value.shape[-1]
    shift %= size
    return value if shift == 0 else pltpu.roll(value, shift, axis=value.ndim - 1)


def tab(tref, name, pos=0):
    return tref[pl.ds((TINDEX[name] + pos) * SUB, SUB), :]


def lane_ds(chunk):
    if isinstance(chunk, int):
        return pl.ds(chunk * LANES, LANES)
    return pl.ds(pl.multiple_of(chunk * LANES, LANES), LANES)


def for_tiles(geo, body):
    def step(pos, carry):
        if geo.chunks == 1:
            body(pos, 0)
        else:
            body(pos // geo.chunks, pos % geo.chunks)
        return carry

    lax.fori_loop(0, geo.nz * geo.chunks, step, 0)


def rows8(pos):
    if isinstance(pos, int):
        return pl.ds(pos * SUB, SUB)
    return pl.ds(pl.multiple_of(pos * SUB, SUB), SUB)


def wide_load(ref, zb, rows, geo):
    parts = [ref[zb, ch, rows, :] for ch in range(geo.chunks)]
    return parts[0] if len(parts) == 1 else jnp.concatenate(parts, axis=1)


def wide_store(ref, zb, rows, geo, value):
    for ch in range(geo.chunks):
        ref[zb, ch, rows, :] = value[:, ch * LANES : (ch + 1) * LANES]


def gather_sum(ref, mref, geo, n):
    xs = geo.wy * geo.cz
    last = (n - 1) * n
    for b in range(n):
        for zb in range(geo.nz):
            low = wide_load(ref, zb, rows8(b), geo)
            high = wide_load(ref, zb, rows8(last + b), geo)
            wide_store(ref, zb, rows8(b), geo, low + roll(high, xs))
            wide_store(ref, zb, rows8(last + b), geo, high + roll(low, -xs))
    y_lo = mref[MASK_Y_LO : MASK_Y_LO + 1, :]
    y_hi = mref[MASK_Y_HI : MASK_Y_HI + 1, :]
    for a in range(n):
        first, final = rows8(a * n), rows8(a * n + n - 1)
        for zb in range(geo.nz):
            low = wide_load(ref, zb, first, geo)
            high = wide_load(ref, zb, final, geo)
            wide_store(ref, zb, first, geo, low + y_lo * roll(high, geo.cz))
            wide_store(ref, zb, final, geo, high + y_hi * roll(low, -geo.cz))
    z_lo = mref[MASK_Z_LO : MASK_Z_LO + 1, :] > 0.5
    z_hi = mref[MASK_Z_HI : MASK_Z_HI + 1, :] > 0.5
    group = min(SUB, n * n)
    for g in range(n * n // group):
        first = pl.ds(g * group * SUB, group, stride=SUB)
        final = pl.ds(g * group * SUB + n - 1, group, stride=SUB)
        low = [wide_load(ref, zb, first, geo) for zb in range(geo.nz)]
        high = [wide_load(ref, zb, final, geo) for zb in range(geo.nz)]
        for zb in range(geo.nz):
            before = roll(high[(zb - 1) % geo.nz], -(geo.cz - 1))
            after = roll(low[(zb + 1) % geo.nz], geo.cz - 1)
            near = jnp.where(z_lo, roll(high[zb], 1), before)
            wide_store(ref, zb, first, geo, low[zb] + near)
            near = jnp.where(z_hi, roll(low[zb], -1), after)
            wide_store(ref, zb, final, geo, high[zb] + near)


def contract(values, level):
    half = level.n // 2
    sums = [values[a] + values[level.n - 1 - a] for a in range(half)]
    diffs = [values[a] - values[level.n - 1 - a] for a in range(half)]
    out = [None] * level.n
    for i in range(half):
        even = sums[0] * level.even[i][0]
        odd = diffs[0] * level.odd[i][0]
        for a in range(1, half):
            even = even + sums[a] * level.even[i][a]
            odd = odd + diffs[a] * level.odd[i][a]
        out[i] = even + odd
        out[level.n - 1 - i] = even - odd
    return out


def combine(values, table):
    out = []
    for i in range(table.shape[0]):
        total = values[0] * float(table[i, 0])
        for a in range(1, table.shape[1]):
            total = total + values[a] * float(table[i, a])
        out.append(total)
    return out


def sublane_mix(ref, zb, ch, row, columns):
    total = ref[zb, ch, pl.ds(row, 1), :] * columns[0]
    for c in range(1, len(columns)):
        total = total + ref[zb, ch, pl.ds(row + c, 1), :] * columns[c]
    return total


def apply_local(src, dst, gref, tref, geo, level):
    n = level.n
    kname, wname = ("kz8", "w8") if n == NF else ("kz4", "w4")

    def body(zb, ch):
        ln = lane_ds(ch)
        wc = tab(tref, wname)
        gw = [gref[zb, ch, pl.ds(i, 1), :] * wc for i in range(3)]
        columns = [tab(tref, kname, c) for c in range(n)]
        for b in range(n):
            mixed = contract([src[zb, ch, rows8(a * n + b), :] for a in range(n)], level)
            for a in range(n):
                dst[zb, ch, rows8(a * n + b), :] = mixed[a] * gw[0]
        for a in range(n):
            mixed = contract([src[zb, ch, rows8(a * n + b), :] for b in range(n)], level)
            for b in range(n):
                row = (a * n + b) * SUB
                along = sublane_mix(src, zb, ch, row, columns)
                total = dst[zb, ch, rows8(a * n + b), :] + mixed[b] * gw[1] + along * gw[2]
                dst[zb, ch, rows8(a * n + b), :] = total * (level.w[a] * level.w[b])

    for_tiles(geo, body)


def local_diagonal(dst, gref, tref, geo, level):
    n = level.n
    wname, dname = ("w8", "kd8") if n == NF else ("w4", "kd4")

    def body(zb, ch):
        ln = lane_ds(ch)
        wc = tab(tref, wname)
        gx = gref[zb, ch, pl.ds(0, 1), :] * wc
        gy = gref[zb, ch, pl.ds(1, 1), :] * wc
        gz = gref[zb, ch, pl.ds(2, 1), :] * tab(tref, dname)
        for a in range(n):
            for b in range(n):
                dst[zb, ch, rows8(a * n + b), :] = (
                    gx * (level.kd[a] * level.w[b])
                    + gy * (level.w[a] * level.kd[b])
                    + gz * (level.w[a] * level.w[b])
                )

    for_tiles(geo, body)


def each_row(geo, n, body):
    def tile(zb, ch):
        for row in range(n * n):
            body(zb, ch, rows8(row))

    for_tiles(geo, tile)


def scales(ref, level):
    return ref[2 * level : 2 * level + 1, :], ref[2 * level + 1 : 2 * level + 2, :]


def first_smooth(res, inv, cur, tmp, mref, gref, tref, geo, level, top):
    first, second = top

    def start(zb, ch, row):
        value = 1.0 / tmp[zb, ch, row, :]
        inv[zb, ch, row, :] = value
        cur[zb, ch, row, :] = value * res[zb, ch, row, :] * first

    each_row(geo, level.n, start)
    apply_local(cur, tmp, gref, tref, geo, level)
    gather_sum(tmp, mref, geo, level.n)

    def finish(zb, ch, row):
        left = res[zb, ch, row, :] - tmp[zb, ch, row, :]
        cur[zb, ch, row, :] = (1.0 + RHO0 * RHO1) * cur[zb, ch, row, :] + second * (
            inv[zb, ch, row, :] * left
        )

    each_row(geo, level.n, finish)
    apply_local(cur, tmp, gref, tref, geo, level)
    gather_sum(tmp, mref, geo, level.n)


def next_smooth(res, inv, cur, step, tmp, mref, gref, tref, geo, level, top):
    first, second = top
    apply_local(cur, tmp, gref, tref, geo, level)
    gather_sum(tmp, mref, geo, level.n)

    def start(zb, ch, row):
        value = inv[zb, ch, row, :] * (res[zb, ch, row, :] - tmp[zb, ch, row, :]) * first
        step[zb, ch, row, :] = value
        cur[zb, ch, row, :] = cur[zb, ch, row, :] + value

    each_row(geo, level.n, start)
    apply_local(cur, tmp, gref, tref, geo, level)
    gather_sum(tmp, mref, geo, level.n)

    def finish(zb, ch, row):
        left = res[zb, ch, row, :] - tmp[zb, ch, row, :]
        cur[zb, ch, row, :] = (
            cur[zb, ch, row, :]
            + (RHO0 * RHO1) * step[zb, ch, row, :]
            + second * (inv[zb, ch, row, :] * left)
        )

    each_row(geo, level.n, finish)


def restrict(res, tmp, dst, mref, tref, geo, nf, nc, table, name, buf):
    scaled = shared_faces(table)

    def body(zb, ch):
        ln = lane_ds(ch)
        f_lo = mref[FAC_Y_LO : FAC_Y_LO + 1, ln]
        f_hi = mref[FAC_Y_HI : FAC_Y_HI + 1, ln]
        part = []
        for b in range(nf):
            values = []
            for a in range(nf):
                row = rows8(a * nf + b)
                values.append(res[zb, ch, row, :] - tmp[zb, ch, row, :])
            mixed = combine(values, scaled.T)
            if b == 0:
                mixed = [v * f_lo for v in mixed]
            if b == nf - 1:
                mixed = [v * f_hi for v in mixed]
            part.append(mixed)
        columns = [tab(tref, name, c) for c in range(nf)]
        for i in range(nc):
            along = combine([part[b][i] for b in range(nf)], table.T)
            for j in range(nc):
                buf[0, 0, rows8(i * nc + j), :] = along[j]
        for row in range(nc * nc):
            dst[zb, ch, rows8(row), :] = sublane_mix(buf, 0, 0, row * SUB, columns)

    for_tiles(geo, body)


def prolong_add(src, base, cur, tref, geo, nf, nc, table, name):
    def body(zb, ch):
        ln = lane_ds(ch)
        columns = [tab(tref, name, c) for c in range(nc)]
        part = []
        for a in range(nc):
            deep = [
                sublane_mix(src, zb, ch, (a * nc + b) * SUB, columns) for b in range(nc)
            ]
            part.append(combine(deep, table))
        for b in range(nf):
            mixed = combine([part[a][b] for a in range(nc)], table)
            for a in range(nf):
                row = rows8(a * nf + b)
                cur[zb, ch, row, :] = base[zb, ch, row, :] + mixed[a]

    for_tiles(geo, body)


def split(value):
    high = value.astype(jnp.bfloat16)
    return high, (value - high.astype(jnp.float32)).astype(jnp.bfloat16)


def dot(left, right, dims):
    return lax.dot_general(left, right, (dims, ((), ())), preferred_element_type=jnp.float32)


def dot3(left, right_high, right_low, dims):
    high, low = split(left)
    return dot(high, right_high, dims) + (dot(high, right_low, dims) + dot(low, right_high, dims))


def pieces_of(own, par, geo):
    my_x = lax.axis_index("gx")
    my_y = lax.axis_index("gy")
    my_h = my_y // geo.cores
    my_c = my_y % geo.cores

    def piece(ix, iy, start, size):
        rel = lax.rem(ix - my_x + geo.gx, geo.gx) * geo.half + lax.rem(
            iy // geo.cores - my_h + geo.half, geo.half
        )
        mine = own[rel, pl.ds(start, size), :]
        if geo.cores == 1:
            return mine
        return jnp.where(my_c == iy % geo.cores, mine, par[rel, pl.ds(start, size), :])

    return piece


def pack_kernel(
    residual, geometry, factor, ids, eig, block, rows, keep, give, scale, metric, names, tops,
    sems, *, geo,
):
    words = NF**3 // LANES
    nblk = ids.shape[-1]
    base, kept, given = rows.shape[0], keep.shape[0], nblk * geo.cz - keep.shape[0]
    pieces = [
        (
            residual.at[:, pl.ds(blk * LANES, LANES)],
            block.at[pl.ds(blk * geo.ne, geo.ne), :],
        )
        for blk in range(words)
    ]
    pieces += [
        (geometry, metric),
        (ids, names),
        (eig, tops),
        (factor.at[pl.ds(0, base), :], rows),
        (factor.at[pl.ds(base, kept), :], keep),
        (factor.at[pl.ds(base + kept, given), :], give.at[pl.ds(0, given), :]),
    ]
    copies = [
        pltpu.make_async_copy(source, target, sems.at[pos])
        for pos, (source, target) in enumerate(pieces)
    ]
    for copy in copies:
        copy.start()
    if given < kept:
        give[pl.ds(given, kept - given), :] = jnp.zeros((kept - given, LANES), jnp.float32)
    for copy in copies:
        copy.wait()
    lines = []
    for level in range(2):
        lines.append(jnp.full((1, LANES), 1.0 / (0.55 * tops[level]), jnp.float32))
        lines.append(jnp.full((1, LANES), 2.0 * RHO1 / (0.45 * tops[level]), jnp.float32))
    lines.append(jnp.zeros((SUB - 4, LANES), jnp.float32))
    scale[...] = jnp.concatenate(lines, axis=0)
    factors = [metric[:, 0, y, :] for y in range(geo.cy)]
    factors.append(jnp.zeros((3, LANES - geo.ne), jnp.float32))
    line = names[0, 0].astype(jnp.float32)
    line = jnp.concatenate([line, jnp.zeros((1, LANES - nblk), jnp.float32)], axis=1)
    block[pl.ds(words * geo.ne, SUB), :] = jnp.concatenate(
        [jnp.concatenate(factors, axis=1), line, jnp.zeros((SUB - 4, LANES), jnp.float32)],
        axis=0,
    )


def mark_kernel(value, out):
    out[...] = value[...]


def factor_kernel(own, par, xhi, xlo, *, geo, nblk, everywhere):
    piece = pieces_of(own, par, geo)
    devices = [(ix, iy) for ix in range(geo.gx) for iy in range(geo.gy)]
    size = own.shape[1] // (geo.nz if everywhere else 1)
    blocks = range(geo.nz if everywhere else 1)
    kept = (nblk + 1) // 2
    tops = geo.cy * nblk * geo.cz

    def top(zb, ix, k):
        side, pos = (1, k) if k < kept else (2, k - kept)
        return piece(ix, geo.gy - side, zb * size + tops + pos * geo.cz, geo.cz)

    for k in range(nblk):
        rows = [
            piece(ix, iy, zb * size + (slot * nblk + k) * geo.cz, geo.cz)
            for zb in blocks
            for ix, iy in devices
            for slot in range(geo.cy)
        ]
        for ix in range(geo.gx):
            for y in range(geo.wy):
                zb = geo.wy - 1 - y
                if zb in blocks:
                    rows.append(top(zb, ix, k))
                else:
                    rows.append(jnp.zeros((geo.cz, LANES), jnp.float32))
        high, rest = split(jnp.concatenate(rows, axis=0))
        xhi[k] = high
        xlo[k] = rest


def fine_kernel(
    own, par, eig, mref, tref, res, inv, cur, resm, gref, labels, tmp, buf, *, geo, prow, everywhere
):
    piece = pieces_of(own, par, geo)
    devices = [(ix, iy) for ix in range(geo.gx) for iy in range(geo.gy)]
    per_chunk = LANES // geo.ne
    words = NF**3 // LANES
    for zb in range(geo.nz):
        for ch in range(geo.chunks):
            group = devices[ch * per_chunk : (ch + 1) * per_chunk]
            for blk in range(words):
                rows = [piece(ix, iy, zb * prow + blk * geo.ne, geo.ne) for ix, iy in group]
                square = jnp.concatenate(rows, axis=0)
                res[zb, ch, pl.ds(blk * LANES, LANES), :] = square.T
            total = None
            for pos, (ix, iy) in enumerate(group):
                part = piece(ix, iy, zb * prow + words * geo.ne, SUB)
                if everywhere or zb == geo.mid:
                    row = (zb if everywhere else 0) * geo.planes + ix * geo.gy + iy
                    labels[pl.ds(row, 1), :] = part[3:4]
                part = roll(part, pos * geo.ne)
                total = part if total is None else total + part
            gref[zb, ch] = total
    gather_sum(res, mref, geo, NF)
    local_diagonal(tmp, gref, tref, geo, FINE)
    gather_sum(tmp, mref, geo, NF)
    first_smooth(res, inv, cur, tmp, mref, gref, tref, geo, FINE, scales(eig, 0))
    restrict(res, tmp, resm, mref, tref, geo, NF, NM, UP_F, "rz8", buf)
    gather_sum(resm, mref, geo, NM)


def merge(src, dst, mref, geo):
    def body(pos):
        pos = pl.multiple_of(pos * SUB, SUB)
        for ch in range(geo.chunks):
            low_half = mref[NEXT_Z : NEXT_Z + 1, lane_ds(ch)] > 0.5
            row = pl.ds(pos, SUB)
            dst[0, ch, row, :] = src[geo.mid, ch, row, :]
            dst[1, ch, row, :] = jnp.where(
                low_half, src[geo.mid + 1, ch, row, :], src[geo.mid - 1, ch, row, :]
            )

    count = src.shape[2] // SUB
    lax.fori_loop(0, count, lambda pos, carry: (body(pos), carry)[1], 0, unroll=min(count, 16))


def middle_kernel(*refs, geo, everywhere):
    res, inv, cur, resm, gref, eig, mref, tref = refs[:8]
    merged, owned = refs[8:15], refs[15]
    invm, curm, tmpm, low, buf = refs[16:]
    local_diagonal(tmpm, gref, tref, geo, MID)
    gather_sum(tmpm, mref, geo, NM)
    first_smooth(resm, invm, curm, tmpm, mref, gref, tref, geo, MID, scales(eig, 1))
    restrict(resm, tmpm, low, mref, tref, geo, NM, NC, UP_C, "rz4", buf)
    z_lo = mref[MASK_Z_LO : MASK_Z_LO + 1, :] > 0.5
    y_lo = mref[MASK_Y_LO : MASK_Y_LO + 1, :]
    top = mref[TOP_ROW : TOP_ROW + 1, :]
    xs = geo.wy * geo.cz

    def node(zb, a, b, c):
        return wide_load(low, zb, pl.ds((a * NC + b) * SUB + c, 1), geo)

    def along_z(zb, a, b):
        before = roll(node((zb - 1) % geo.nz, a, b, 1), -(geo.cz - 1))
        return node(zb, a, b, 0) + jnp.where(z_lo, roll(node(zb, a, b, 1), 1), before)

    tops = None
    blocks = range(geo.nz) if everywhere else [geo.mid]
    for pos, zb in enumerate(blocks):
        grid = [[along_z(zb, a, b) for b in range(NC)] for a in range(NC)]
        floor = [grid[a][0] + y_lo * roll(grid[a][1], geo.cz) for a in range(NC)]
        owned[:, pl.ds(pos * geo.lanes, geo.lanes)] = jnp.broadcast_to(
            floor[0] + roll(floor[1], xs), (SUB, geo.lanes)
        )
        ceil = top * (grid[0][1] + roll(grid[1][1], xs))
        ceil = roll(ceil, -geo.cz * pos)
        tops = ceil if tops is None else tops + ceil
    owned[:, pl.ds(len(blocks) * geo.lanes, geo.lanes)] = jnp.broadcast_to(
        tops, (SUB, geo.lanes)
    )
    for source, target in zip((res, inv, cur, resm, invm, curm, gref), merged):
        merge(source, target, mref, geo)


def owner_mask(owners, count):
    width = owners.shape[1]
    row = lax.broadcasted_iota(jnp.int32, (count, width), 0).astype(jnp.float32)
    return jnp.broadcast_to(owners[0:1, :], (count, width)) == row


def contributions(owned, owners, xhi, xlo, nblk, count):
    spread = jnp.broadcast_to(owned[0:1, :], (count, owned.shape[1]))
    spread = jnp.where(owner_mask(owners, count), spread, 0.0)
    return [dot3(spread, xhi[k], xlo[k], ((1,), (0,))) for k in range(nblk)]


def pick_columns(values, labels, own_labels, nblk):
    count = own_labels.shape[0]
    every = labels.shape[0]
    id_rows = jnp.concatenate([own_labels[:, k : k + 1] for k in range(nblk)], axis=0)
    picked = None
    per_step = nblk if nblk * every <= 1024 else 1
    for k0 in range(0, nblk, per_step):
        ks = range(k0, k0 + per_step)
        cols = jnp.concatenate([labels[:, k : k + 1] for k in ks], axis=0)
        id_lanes = jnp.broadcast_to(cols, (cols.shape[0], LANES)).T[0:1]
        hit = (id_rows == id_lanes).astype(jnp.bfloat16)
        high, rest = split(jnp.concatenate([values[k] for k in ks], axis=0))
        part = dot(hit, high, ((1,), (0,))) + dot(hit, rest, ((1,), (0,)))
        picked = part if picked is None else picked + part
    return [picked[k * count : (k + 1) * count] for k in range(nblk)]


def solve_rows(picked, owners, xhi, xlo):
    full = None
    for k, value in enumerate(picked):
        part = dot3(value, xhi[k], xlo[k], ((1,), (1,)))
        full = part if full is None else full + part
    mine = owner_mask(owners, full.shape[0])
    return jnp.sum(jnp.where(mine, full, 0.0), axis=0, keepdims=True)


def send_kernel(owned, owners, xhi, xlo, labels, send, *, geo, nblk):
    for k, value in enumerate(contributions(owned, owners, xhi, xlo, nblk, geo.planes)):
        send[:, pl.ds(k * LANES, LANES)] = value
    send[:, pl.ds(nblk * LANES, LANES)] = labels[...]


def coarse_kernel(*refs, geo, nblk, peers):
    parts = refs[:peers]
    xhi, xlo, owners, out = refs[peers:]
    values = [
        jnp.concatenate([part[:, pl.ds(k * LANES, LANES)] for part in parts], axis=0)
        for k in range(nblk + 1)
    ]
    own_labels = parts[0][:, pl.ds(nblk * LANES, LANES)]
    picked = pick_columns(values[:nblk], values[nblk], own_labels, nblk)
    solved = solve_rows(picked, owners, xhi, xlo)
    out[pl.ds(0, 1), :] = solved[:, : geo.lanes]
    out[pl.ds(1, 1), :] = solved[:, geo.lanes :]


def rise(solved, state, consts, out, scratch, geo):
    res, inv, cur_in, resm, invm, curm_in, gref = state
    eig, mref, tref = consts
    cur, curm, tmp, tmpm, step, stepm, low, turned = scratch
    y_hi = mref[MASK_Y_HI : MASK_Y_HI + 1, :] > 0.5
    z_hi = mref[MASK_Z_HI : MASK_Z_HI + 1, :] > 0.5
    xs = geo.wy * geo.cz
    levels = []
    for base, ceil in solved:
        upper = jnp.where(y_hi, roll(base, -geo.cz), ceil)
        flat = [base, upper]
        levels.append([flat, [roll(v, -xs) for v in flat]])
    low_half = mref[NEXT_Z : NEXT_Z + 1, :] > 0.5
    for a in range(NC):
        for b in range(NC):
            flat = [levels[zb][a][b] for zb in range(3)]
            deep = [
                jnp.where(z_hi, roll(flat[zb], -1), roll(flat[(zb + 1) % 3], geo.cz - 1))
                for zb in range(3)
            ]
            for c, value in enumerate((flat, deep)):
                row = pl.ds((a * NC + b) * SUB + c, 1)
                wide_store(low, 0, row, geo, value[1])
                wide_store(low, 1, row, geo, jnp.where(low_half, value[2], value[0]))
    prolong_add(low, curm_in, curm, tref, geo, NM, NC, UP_C, "pz4")
    next_smooth(resm, invm, curm, stepm, tmpm, mref, gref, tref, geo, MID, scales(eig, 1))
    prolong_add(curm, cur_in, cur, tref, geo, NF, NM, UP_F, "pz8")
    next_smooth(res, inv, cur, step, tmp, mref, gref, tref, geo, FINE, scales(eig, 0))
    words = NF**3 // LANES
    for ch in range(geo.chunks):
        for blk in range(words):
            turned[pl.ds(ch * LANES, LANES), pl.ds(blk * LANES, LANES)] = cur[
                geo.mid, ch, pl.ds(blk * LANES, LANES), :
            ].T
    my = lax.axis_index("gx") * geo.gy + lax.axis_index("gy")
    out[...] = turned[pl.ds(pl.multiple_of(my * geo.ne, SUB), geo.ne), :]


def up_kernel(*refs, geo):
    blocks = [(ref[0:1, :], ref[1:2, :]) for ref in refs[:3]]
    rest = refs[3:]
    rise(blocks, rest[:7], rest[7:10], rest[10], rest[11:], geo)


def finish_kernel(owned, owners, xhi, xlo, labels, *refs, geo, nblk):
    values = contributions(owned, owners, xhi, xlo, nblk, labels.shape[0])
    names = labels[...]
    picked = pick_columns(values, names, names, nblk)
    solved = solve_rows(picked, owners, xhi, xlo)
    near = geo.window(2, 0)
    tops = solved[:, geo.nz * geo.lanes :]
    blocks = [
        (solved[:, zb * geo.lanes : (zb + 1) * geo.lanes], roll(tops, geo.cz * zb))
        for zb in range(3)
    ]
    rise(blocks, refs[:7], refs[7:10], refs[10], refs[11:], near)


def holds_all(gx, gy, gz, cy, cz):
    nodes = gx * gy * gz * cy * cz * NF**3
    return 3 <= gz <= gy * cy and nodes * 4 <= MAX_EVERYWHERE


def on_device(residual_in, geometry, eig_top, coarse_rows, block_ids, sizes, everywhere):
    gx, gy, gz = sizes
    cx, cy, cz = residual_in.shape[:3]
    nblk = coarse_rows.shape[3]
    geo = Geo(gx, gy, cy, cz, 3)
    if everywhere:
        geo = geo.window(gz)
    ok = cx == 1 and cz % SUB == 0 and LANES % geo.ne == 0 and geo.lanes % LANES == 0
    if not ok or coarse_rows.shape[4] != LANES or geo.planes % SUB:
        raise ValueError("block shape")
    f32 = jnp.float32
    vmem = pl.BlockSpec(memory_space=pltpu.VMEM)
    smem = pl.BlockSpec(memory_space=pltpu.SMEM)
    half, cores = geo.half, geo.cores
    slots = (cy + 1) * cz
    prow = NF**3 // LANES * geo.ne + SUB

    def shape(dims, kind=f32):
        return jax.ShapeDtypeStruct(dims, kind)

    def call(body, specs, outs, scratch, *operands, extra=()):
        kept = list(operands) + list(outs) + list(scratch)
        total = sum(math.prod(a.shape) * a.dtype.itemsize for a in kept)
        return pl.pallas_call(
            body,
            out_shape=list(outs),
            in_specs=specs,
            out_specs=[vmem] * len(outs),
            scratch_shapes=[pltpu.VMEM(a.shape, a.dtype) for a in scratch] + list(extra),
            compiler_params=pltpu.CompilerParams(
                vmem_limit_bytes=min(total + (3 << 20), 60 << 20)
            ),
        )(*operands)

    def rank(ix, ih, core):
        return (ix % gx) * gy + (ih % half) * cores + core

    def across_chips(value):
        parts = [value]
        for dx in range(gx):
            for dh in range(half):
                if dx or dh:
                    pairs = [
                        (rank(ix + dx, ih + dh, core), rank(ix, ih, core))
                        for ix in range(gx)
                        for ih in range(half)
                        for core in range(cores)
                    ]
                    parts.append(lax.ppermute(value, ("gx", "gy"), pairs))
        return parts

    def between_cores(value):
        if cores == 1:
            return value
        return lax.ppermute(value, "gy", [(i, i ^ 1) for i in range(gy)])

    hbm = pl.BlockSpec(memory_space=pltpu.HBM)
    factor = coarse_rows.reshape(cy + 1, cz, nblk, LANES).transpose(0, 2, 1, 3)
    part = shape(((nblk + 1) // 2 * cz, LANES))
    block, factor, keep, give, scale = call(
        functools.partial(pack_kernel, geo=geo),
        [hbm] * 5,
        [shape((prow, LANES)), shape((cy * nblk * cz, LANES)), part, part, shape((SUB, LANES))],
        [shape(geometry.shape), jax.ShapeDtypeStruct(block_ids.shape, block_ids.dtype)],
        *[
            pltpu.with_memory_space_constraint(value, pltpu.HBM)
            for value in (
                residual_in.reshape(geo.ne, NF**3),
                geometry,
                factor.reshape(slots * nblk, LANES),
                block_ids,
                eig_top,
            )
        ],
        extra=[pltpu.SMEM((2,), f32), pltpu.SemaphoreType.DMA((NF**3 // LANES + 6,))],
    )
    marks = [call(mark_kernel, [vmem], [shape((SUB, LANES))], [], scale)[0] for _ in range(2)]

    def from_block(value, offset):
        return lax.ppermute(value, "gz", [((i + offset) % gz, i) for i in range(gz)])

    def along_z(value):
        order = list(range(2, geo.nz - 1)) + [-1, 1]
        got = {offset: from_block(value, offset) for offset in order}
        got[0] = value
        return jnp.concatenate([got[offset] for offset in sorted(got)], axis=0)

    taken = lax.ppermute(give, "gy", [(gy - 1, gy - 2)])
    keep = jnp.where(lax.axis_index("gy") == gy - 1, keep, taken)
    factor = jnp.concatenate([factor, keep], axis=0)
    column = along_z(block)
    if everywhere:
        factor = along_z(factor)
    own = jnp.stack(across_chips(column))
    par = between_cores(own)
    factor_own = across_chips(factor)

    masks = jnp.asarray(geo.masks())
    owners = jnp.asarray(geo.owners(everywhere))
    table = jnp.asarray(TABLE)
    count = geo.planes * (geo.nz if everywhere else 1)
    width = owners.shape[1]
    near = geo.window(2, 0)

    def field(where, points):
        return shape((where.nz, where.chunks, points * points * SUB, LANES))

    fine, middle, lowest = (field(geo, points) for points in (NF, NM, NC))
    buf = shape((1, 1, NM * NM * SUB, LANES))
    metric = shape((geo.nz, geo.chunks, SUB, LANES))
    res, inv, cur, resm, gfac, names = call(
        functools.partial(fine_kernel, geo=geo, prow=prow, everywhere=everywhere),
        [vmem] * 5,
        [fine] * 3 + [middle, metric, shape((count, LANES))],
        [fine, buf],
        own, par, marks[1], masks, table,
    )
    factor_par = jnp.stack([between_cores(part) for part in factor_own])
    factor_own = jnp.stack(factor_own)
    fine2, middle2 = (field(near, points) for points in (NF, NM))
    *merged, owned = call(
        functools.partial(middle_kernel, geo=geo, everywhere=everywhere),
        [vmem] * 8,
        [fine2] * 3
        + [middle2] * 3
        + [shape((2, geo.chunks, SUB, LANES)), shape((SUB, width))],
        [middle, middle, middle, lowest, buf],
        res, inv, cur, resm, gfac, marks[0], masks, table,
    )
    wide = shape((nblk, width, LANES), jnp.bfloat16)
    xhi, xlo = call(
        functools.partial(factor_kernel, geo=geo, nblk=nblk, everywhere=everywhere),
        [vmem, vmem],
        [wide, wide],
        [],
        factor_own, factor_par,
    )
    state = (*merged, scale, masks, table)
    kinds = [vmem] * 10
    final = shape((geo.ne, NF**3))
    scratch = [fine2, middle2] * 3 + [field(near, NC), shape((geo.lanes, NF**3))]
    if everywhere:
        (out,) = call(
            functools.partial(finish_kernel, geo=geo, nblk=nblk),
            [vmem] * 5 + kinds,
            [final],
            scratch,
            owned, owners, xhi, xlo, names, *state,
        )
        return out.reshape(cx, cy, cz, NF**3)

    (send,) = call(
        functools.partial(send_kernel, geo=geo, nblk=nblk),
        [vmem] * 5,
        [shape((geo.planes, (nblk + 1) * LANES))],
        [],
        owned, owners, xhi, xlo, names,
    )
    parts = [send] + [from_block(send, offset) for offset in range(1, gz)]
    (solved,) = call(
        functools.partial(coarse_kernel, geo=geo, nblk=nblk, peers=gz),
        [vmem] * (gz + 3),
        [shape((SUB, geo.lanes))],
        [],
        *parts, xhi, xlo, owners,
    )
    (out,) = call(
        functools.partial(up_kernel, geo=geo),
        [vmem] * 3 + kinds,
        [final],
        scratch,
        from_block(solved, -1), solved, from_block(solved, 1), *state,
    )
    return out.reshape(cx, cy, cz, NF**3)


def solution(mesh):
    sizes = tuple(mesh.shape[name] for name in ("gx", "gy", "gz"))
    in_specs = (
        P("gx", "gy", "gz", None),
        P(None, "gx", "gy", "gz"),
        P(),
        P("gx", "gy", "gz", None, None),
        P("gx", "gy", "gz", None),
    )
    out_specs = P("gx", "gy", "gz", None)

    def program(residual_in, geometry, eig_top, coarse_rows, block_ids):
        gx, gy, gz = sizes
        cy, cz = residual_in.shape[1] // gy, residual_in.shape[2] // gz
        everywhere = holds_all(gx, gy, gz, cy, cz)

        def body(*blocks):
            return on_device(*blocks, sizes=sizes, everywhere=everywhere)

        step = jax.shard_map(
            body, mesh=mesh, in_specs=in_specs, out_specs=out_specs, check_vma=False
        )
        return step(residual_in, geometry, eig_top, coarse_rows, block_ids)

    return program
```

```python
import functools
import math

import jax
import jax.numpy as jnp
import numpy as np
from jax import lax
from jax.experimental import pallas as pl
from jax.experimental.pallas import tpu as pltpu
from jax.sharding import PartitionSpec as P


NF = 8
NM = 4
NC = 2
LANES = 128
SUB = 8
MAX_EVERYWHERE = 2 << 20
SIGMA = 0.55 / 0.45
RHO0 = 1.0 / SIGMA
RHO1 = 1.0 / (2.0 * SIGMA - RHO0)


def legendre_pair(point, degree):
    previous = 1.0
    current = point
    for order in range(1, degree):
        following = ((2 * order + 1) * point * current - order * previous) / (order + 1)
        previous = current
        current = following
    return (current, previous)


def gll_tables(points):
    degree = points - 1
    node_list = []
    for index in range(points):
        guess = -math.cos(math.pi * index / degree)
        for _ in range(100):
            high_val, low_val = legendre_pair(guess, degree)
            guess = guess - (guess * high_val - low_val) / (points * high_val)
        node_list.append(guess)
    node_list[0] = -1.0
    node_list[degree] = 1.0
    node_pos = np.array(node_list)
    at_nodes = np.array([legendre_pair(value, degree)[0] for value in node_list])
    weights = 2.0 / (degree * (degree + 1) * at_nodes**2)
    derivative = np.zeros((points, points))
    for row_pos in range(points):
        for col_pos in range(points):
            if row_pos != col_pos:
                derivative[row_pos, col_pos] = at_nodes[row_pos] / (
                    at_nodes[col_pos] * (node_pos[row_pos] - node_pos[col_pos])
                )
    derivative[0, 0] = -degree * (degree + 1) / 4.0
    derivative[degree, degree] = degree * (degree + 1) / 4.0
    stiffness = derivative.T @ (weights[:, None] * derivative)
    return (node_pos, weights, stiffness)


def interp_table(fine_pts, coarse_pts):
    fine_nodes = gll_tables(fine_pts)[0]
    coarse_nodes = gll_tables(coarse_pts)[0]
    lagrange = np.ones((fine_pts, coarse_pts))
    for col_pos in range(coarse_pts):
        for other_pos in range(coarse_pts):
            if other_pos != col_pos:
                lagrange[:, col_pos] *= (fine_nodes - coarse_nodes[other_pos]) / (
                    coarse_nodes[col_pos] - coarse_nodes[other_pos]
                )
    return lagrange


class Level:
    def __init__(self, points):
        self.n = points
        _, weights, stiffness = gll_tables(points)
        self.w = [float(v) for v in weights]
        self.kd = [float(v) for v in np.diag(stiffness)]
        scaled = stiffness / weights[:, None]
        half = points // 2
        flipped = scaled[:, ::-1]
        self.even = [[float(v) for v in row[:half]] for row in (scaled + flipped)[:half] / 2]
        self.odd = [[float(v) for v in row[:half]] for row in (scaled - flipped)[:half] / 2]
        self.scaled = scaled
        self.weights = weights
        self.diag = np.diag(stiffness)


FINE = Level(NF)
MID = Level(NM)
UP_F = interp_table(NF, NM)
UP_C = interp_table(NM, NC)


def shared_faces(lagrange):
    out = lagrange.copy()
    out[0] *= 0.5
    out[-1] *= 0.5
    return out


def pad_rows(column, fill=0.0):
    out = np.full((SUB,), fill)
    out[: column.shape[0]] = column
    return out


def build_tables():
    rows = []
    index = {}

    def put(name, columns):
        index[name] = len(rows)
        rows.extend(columns)

    put("kz8", [FINE.scaled[:, c] for c in range(NF)])
    put("kz4", [pad_rows(MID.scaled[:, c]) for c in range(NM)])
    put("w8", [FINE.weights])
    put("w4", [pad_rows(MID.weights, 1.0)])
    put("kd8", [FINE.diag])
    put("kd4", [pad_rows(MID.diag, 1.0)])
    put("rz8", [pad_rows(shared_faces(UP_F)[c]) for c in range(NF)])
    put("rz4", [pad_rows(shared_faces(UP_C)[c]) for c in range(NM)])
    put("pz8", [UP_F[:, c] for c in range(NM)])
    put("pz4", [pad_rows(UP_C[:, c]) for c in range(NC)])
    flat = np.concatenate(rows).astype(np.float32)
    return np.ascontiguousarray(np.broadcast_to(flat[:, None], (flat.shape[0], LANES))), index


TABLE, TINDEX = build_tables()


def plane_products(level):
    weight = np.diag(level.weights)
    stiff = level.weights[:, None] * level.scaled
    both = np.concatenate([np.kron(stiff, weight), np.kron(weight, stiff)], axis=0)
    both = both.astype(np.float32)
    high = both.astype(jnp.bfloat16)
    low = (both - high.astype(np.float32)).astype(jnp.bfloat16)
    return np.concatenate([high, high, low, low], axis=1)


PLANES = plane_products(FINE)
MASK_Y_LO, MASK_Y_HI, MASK_Z_LO, MASK_Z_HI, FAC_Y_LO, FAC_Y_HI, TOP_ROW, NEXT_Z = range(8)


class Geo:
    def __init__(self, gx, gy, cy, cz, nz):
        self.gx, self.gy, self.cy, self.cz, self.nz = gx, gy, cy, cz, nz
        self.wy = gy * cy
        self.lanes = gx * self.wy * cz
        self.ne = cy * cz
        self.planes = gx * gy
        self.half = gy // 2 if gy % 2 == 0 else gy
        self.cores = gy // self.half
        self.chunks = self.lanes // LANES
        self.mid = 1

    def window(self, nz, mid=1):
        out = Geo(self.gx, self.gy, self.cy, self.cz, nz)
        out.mid = mid
        return out

    def owners(self, everywhere):
        blocks = self.nz if everywhere else 1
        width = (blocks + 1) * self.lanes
        place = lax.broadcasted_iota(jnp.int32, (1, width), 1)
        base = lax.shift_right_logical(place, self.ne.bit_length() - 1)
        rest = place - blocks * self.lanes
        y = lax.shift_right_logical(rest, self.cz.bit_length() - 1) & (self.wy - 1)
        x = lax.shift_right_logical(rest, (self.cz * self.wy).bit_length() - 1)
        zb = self.wy - 1 - y
        top = jnp.where(zb < blocks, zb * self.planes + x * self.gy + self.gy - 1, -1)
        return jnp.where(rest < 0, base, top)

    def masks(self):
        lane = np.arange(self.lanes)
        z = lane % self.cz
        y = (lane // self.cz) % self.wy
        out = np.zeros((8, self.lanes), np.float32)
        out[MASK_Y_LO] = y > 0
        out[MASK_Y_HI] = y < self.wy - 1
        out[MASK_Z_LO] = z > 0
        out[MASK_Z_HI] = z < self.cz - 1
        out[FAC_Y_LO] = np.where(y > 0, 0.5, 1.0)
        out[FAC_Y_HI] = np.where(y < self.wy - 1, 0.5, 1.0)
        out[TOP_ROW] = y == self.wy - 1
        out[NEXT_Z] = z < self.cz // 2
        return out


def roll(value, shift):
    size = value.shape[-1]
    shift %= size
    return value if shift == 0 else pltpu.roll(value, shift, axis=value.ndim - 1)


def tab(tref, name, pos=0):
    return tref[pl.ds((TINDEX[name] + pos) * SUB, SUB), :]


def lane_ds(chunk):
    if isinstance(chunk, int):
        return pl.ds(chunk * LANES, LANES)
    return pl.ds(pl.multiple_of(chunk * LANES, LANES), LANES)


def for_tiles(geo, body):
    def step(pos, carry):
        if geo.chunks == 1:
            body(pos, 0)
        else:
            body(pos // geo.chunks, pos % geo.chunks)
        return carry

    lax.fori_loop(0, geo.nz * geo.chunks, step, 0)


def rows8(pos):
    if isinstance(pos, int):
        return pl.ds(pos * SUB, SUB)
    return pl.ds(pl.multiple_of(pos * SUB, SUB), SUB)


def wide_load(ref, zb, rows, geo):
    parts = [ref[zb, ch, rows, :] for ch in range(geo.chunks)]
    return parts[0] if len(parts) == 1 else jnp.concatenate(parts, axis=1)


def wide_store(ref, zb, rows, geo, value):
    for ch in range(geo.chunks):
        ref[zb, ch, rows, :] = value[:, ch * LANES : (ch + 1) * LANES]


def gather_sum(ref, mref, geo, n):
    xs = geo.wy * geo.cz
    last = (n - 1) * n
    for b in range(n):
        for zb in range(geo.nz):
            low = wide_load(ref, zb, rows8(b), geo)
            high = wide_load(ref, zb, rows8(last + b), geo)
            wide_store(ref, zb, rows8(b), geo, low + roll(high, xs))
            wide_store(ref, zb, rows8(last + b), geo, high + roll(low, -xs))
    y_lo = mref[MASK_Y_LO : MASK_Y_LO + 1, :]
    y_hi = mref[MASK_Y_HI : MASK_Y_HI + 1, :]
    for a in range(n):
        first, final = rows8(a * n), rows8(a * n + n - 1)
        for zb in range(geo.nz):
            low = wide_load(ref, zb, first, geo)
            high = wide_load(ref, zb, final, geo)
            wide_store(ref, zb, first, geo, low + y_lo * roll(high, geo.cz))
            wide_store(ref, zb, final, geo, high + y_hi * roll(low, -geo.cz))
    z_lo = mref[MASK_Z_LO : MASK_Z_LO + 1, :] > 0.5
    z_hi = mref[MASK_Z_HI : MASK_Z_HI + 1, :] > 0.5
    group = min(SUB, n * n)
    for g in range(n * n // group):
        first = pl.ds(g * group * SUB, group, stride=SUB)
        final = pl.ds(g * group * SUB + n - 1, group, stride=SUB)
        low = [wide_load(ref, zb, first, geo) for zb in range(geo.nz)]
        high = [wide_load(ref, zb, final, geo) for zb in range(geo.nz)]
        for zb in range(geo.nz):
            before = roll(high[(zb - 1) % geo.nz], -(geo.cz - 1))
            after = roll(low[(zb + 1) % geo.nz], geo.cz - 1)
            near = jnp.where(z_lo, roll(high[zb], 1), before)
            wide_store(ref, zb, first, geo, low[zb] + near)
            near = jnp.where(z_hi, roll(low[zb], -1), after)
            wide_store(ref, zb, final, geo, high[zb] + near)


def contract(values, level):
    half = level.n // 2
    sums = [values[a] + values[level.n - 1 - a] for a in range(half)]
    diffs = [values[a] - values[level.n - 1 - a] for a in range(half)]
    out = [None] * level.n
    for i in range(half):
        even = sums[0] * level.even[i][0]
        odd = diffs[0] * level.odd[i][0]
        for a in range(1, half):
            even = even + sums[a] * level.even[i][a]
            odd = odd + diffs[a] * level.odd[i][a]
        out[i] = even + odd
        out[level.n - 1 - i] = even - odd
    return out


def combine(values, table):
    out = []
    for i in range(table.shape[0]):
        total = values[0] * float(table[i, 0])
        for a in range(1, table.shape[1]):
            total = total + values[a] * float(table[i, a])
        out.append(total)
    return out


def sublane_mix(ref, zb, ch, row, columns):
    total = ref[zb, ch, pl.ds(row, 1), :] * columns[0]
    for c in range(1, len(columns)):
        total = total + ref[zb, ch, pl.ds(row + c, 1), :] * columns[c]
    return total


def apply_fine(src, dst, gref, tref, pref, geo):
    level = FINE
    n = level.n

    def body(zb, ch):
        wc = tab(tref, "w8")
        g0, g1, g2 = [gref[zb, ch, pl.ds(i, 1), :] for i in range(3)]
        gw = g0 * wc
        for b in range(n):
            mixed = contract([src[zb, ch, rows8(a * n + b), :] for a in range(n)], level)
            factors = [gw * (level.w[b] * level.w[a]) for a in range(n // 2)]
            for a in range(n):
                dst[zb, ch, rows8(a * n + b), :] = mixed[a] * factors[min(a, n - 1 - a)]
        planes = pref[...]
        for a in range(n):
            slab = pl.ds(a * n * SUB, n * SUB)
            high, low = split(src[zb, ch, slab, :])
            data = jnp.concatenate([high, low, high, low], axis=0)
            both = dot(planes, data, ((1,), (0,)))
            total = both[: n * SUB] * g1 + both[n * SUB :] * g2
            dst[zb, ch, slab, :] = (dst[zb, ch, slab, :] + total * level.w[a])

    for_tiles(geo, body)


def apply_middle(src, dst, gref, tref, geo):
    level = MID
    n = level.n
    kname, wname = "kz4", "w4"

    def body(zb, ch):
        ln = lane_ds(ch)
        wc = tab(tref, wname)
        gw = [gref[zb, ch, pl.ds(i, 1), :] * wc for i in range(3)]
        columns = [tab(tref, kname, c) for c in range(n)]
        for b in range(n):
            mixed = contract([src[zb, ch, rows8(a * n + b), :] for a in range(n)], level)
            for a in range(n):
                dst[zb, ch, rows8(a * n + b), :] = mixed[a] * gw[0]
        for a in range(n):
            mixed = contract([src[zb, ch, rows8(a * n + b), :] for b in range(n)], level)
            for b in range(n):
                row = (a * n + b) * SUB
                along = sublane_mix(src, zb, ch, row, columns)
                total = dst[zb, ch, rows8(a * n + b), :] + mixed[b] * gw[1] + along * gw[2]
                dst[zb, ch, rows8(a * n + b), :] = total * (level.w[a] * level.w[b])

    for_tiles(geo, body)


def local_diagonal(dst, gref, tref, geo, level):
    n = level.n
    wname, dname = ("w8", "kd8") if n == NF else ("w4", "kd4")

    def body(zb, ch):
        ln = lane_ds(ch)
        wc = tab(tref, wname)
        gx = gref[zb, ch, pl.ds(0, 1), :] * wc
        gy = gref[zb, ch, pl.ds(1, 1), :] * wc
        gz = gref[zb, ch, pl.ds(2, 1), :] * tab(tref, dname)
        for a in range(n):
            for b in range(n):
                dst[zb, ch, rows8(a * n + b), :] = (
                    gx * (level.kd[a] * level.w[b])
                    + gy * (level.w[a] * level.kd[b])
                    + gz * (level.w[a] * level.w[b])
                )

    for_tiles(geo, body)


def each_row(geo, n, body):
    def tile(zb, ch):
        for row in range(n * n):
            body(zb, ch, rows8(row))

    for_tiles(geo, tile)


def scales(ref, level):
    return ref[2 * level : 2 * level + 1, :], ref[2 * level + 1 : 2 * level + 2, :]


def first_smooth(res, inv, cur, tmp, mref, geo, level, top, operate):
    first, second = top

    def start(zb, ch, row):
        value = 1.0 / tmp[zb, ch, row, :]
        inv[zb, ch, row, :] = value
        cur[zb, ch, row, :] = value * res[zb, ch, row, :] * first

    each_row(geo, level.n, start)
    operate(cur, tmp)
    gather_sum(tmp, mref, geo, level.n)

    def finish(zb, ch, row):
        left = res[zb, ch, row, :] - tmp[zb, ch, row, :]
        cur[zb, ch, row, :] = (1.0 + RHO0 * RHO1) * cur[zb, ch, row, :] + second * (
            inv[zb, ch, row, :] * left
        )

    each_row(geo, level.n, finish)
    operate(cur, tmp)
    gather_sum(tmp, mref, geo, level.n)


def next_smooth(res, inv, cur, step, tmp, mref, geo, level, top, operate):
    first, second = top
    operate(cur, tmp)
    gather_sum(tmp, mref, geo, level.n)

    def start(zb, ch, row):
        value = inv[zb, ch, row, :] * (res[zb, ch, row, :] - tmp[zb, ch, row, :]) * first
        step[zb, ch, row, :] = value
        cur[zb, ch, row, :] = cur[zb, ch, row, :] + value

    each_row(geo, level.n, start)
    operate(cur, tmp)
    gather_sum(tmp, mref, geo, level.n)

    def finish(zb, ch, row):
        left = res[zb, ch, row, :] - tmp[zb, ch, row, :]
        cur[zb, ch, row, :] = (
            cur[zb, ch, row, :]
            + (RHO0 * RHO1) * step[zb, ch, row, :]
            + second * (inv[zb, ch, row, :] * left)
        )

    each_row(geo, level.n, finish)


def restrict(res, tmp, dst, mref, tref, geo, nf, nc, table, name, buf):
    scaled = shared_faces(table)

    def body(zb, ch):
        ln = lane_ds(ch)
        f_lo = mref[FAC_Y_LO : FAC_Y_LO + 1, ln]
        f_hi = mref[FAC_Y_HI : FAC_Y_HI + 1, ln]
        part = []
        for b in range(nf):
            values = []
            for a in range(nf):
                row = rows8(a * nf + b)
                values.append(res[zb, ch, row, :] - tmp[zb, ch, row, :])
            mixed = combine(values, scaled.T)
            if b == 0:
                mixed = [v * f_lo for v in mixed]
            if b == nf - 1:
                mixed = [v * f_hi for v in mixed]
            part.append(mixed)
        columns = [tab(tref, name, c) for c in range(nf)]
        for i in range(nc):
            along = combine([part[b][i] for b in range(nf)], table.T)
            for j in range(nc):
                buf[0, 0, rows8(i * nc + j), :] = along[j]
        for row in range(nc * nc):
            dst[zb, ch, rows8(row), :] = sublane_mix(buf, 0, 0, row * SUB, columns)

    for_tiles(geo, body)


def prolong_add(src, base, cur, tref, geo, nf, nc, table, name):
    def body(zb, ch):
        ln = lane_ds(ch)
        columns = [tab(tref, name, c) for c in range(nc)]
        part = []
        for a in range(nc):
            deep = [
                sublane_mix(src, zb, ch, (a * nc + b) * SUB, columns) for b in range(nc)
            ]
            part.append(combine(deep, table))
        for b in range(nf):
            mixed = combine([part[a][b] for a in range(nc)], table)
            for a in range(nf):
                row = rows8(a * nf + b)
                cur[zb, ch, row, :] = base[zb, ch, row, :] + mixed[a]

    for_tiles(geo, body)


def split(value):
    high = value.astype(jnp.bfloat16)
    return high, (value - high.astype(jnp.float32)).astype(jnp.bfloat16)


def dot(left, right, dims):
    return lax.dot_general(left, right, (dims, ((), ())), preferred_element_type=jnp.float32)


def dot3(left, right_high, right_low, dims):
    high, low = split(left)
    return dot(high, right_high, dims) + (dot(high, right_low, dims) + dot(low, right_high, dims))


def pieces_of(own, par, geo):
    my_x = lax.axis_index("gx")
    my_y = lax.axis_index("gy")
    my_h = my_y // geo.cores
    my_c = my_y % geo.cores

    def piece(ix, iy, start, size):
        rel = lax.rem(ix - my_x + geo.gx, geo.gx) * geo.half + lax.rem(
            iy // geo.cores - my_h + geo.half, geo.half
        )
        mine = own[rel, pl.ds(start, size), :]
        if geo.cores == 1:
            return mine
        return jnp.where(my_c == iy % geo.cores, mine, par[rel, pl.ds(start, size), :])

    return piece


def pack_kernel(
    residual, geometry, factor, ids, eig, block, rows, keep, give, scale, metric, names, tops,
    sems, *, geo,
):
    words = NF**3 // LANES
    nblk = ids.shape[-1]
    base, kept, given = rows.shape[0], keep.shape[0], nblk * geo.cz - keep.shape[0]
    pieces = [
        (
            residual.at[:, pl.ds(blk * LANES, LANES)],
            block.at[pl.ds(blk * geo.ne, geo.ne), :],
        )
        for blk in range(words)
    ]
    pieces += [
        (geometry, metric),
        (ids, names),
        (eig, tops),
        (factor.at[pl.ds(0, base), :], rows),
        (factor.at[pl.ds(base, kept), :], keep),
        (factor.at[pl.ds(base + kept, given), :], give.at[pl.ds(0, given), :]),
    ]
    copies = [
        pltpu.make_async_copy(source, target, sems.at[pos])
        for pos, (source, target) in enumerate(pieces)
    ]
    for copy in copies:
        copy.start()
    if given < kept:
        give[pl.ds(given, kept - given), :] = jnp.zeros((kept - given, LANES), jnp.float32)
    for copy in copies:
        copy.wait()
    lines = []
    for level in range(2):
        lines.append(jnp.full((1, LANES), 1.0 / (0.55 * tops[level]), jnp.float32))
        lines.append(jnp.full((1, LANES), 2.0 * RHO1 / (0.45 * tops[level]), jnp.float32))
    lines.append(jnp.zeros((SUB - 4, LANES), jnp.float32))
    scale[...] = jnp.concatenate(lines, axis=0)
    factors = [metric[:, 0, y, :] for y in range(geo.cy)]
    factors.append(jnp.zeros((3, LANES - geo.ne), jnp.float32))
    line = names[0, 0].astype(jnp.float32)
    line = jnp.concatenate([line, jnp.zeros((1, LANES - nblk), jnp.float32)], axis=1)
    block[pl.ds(words * geo.ne, SUB), :] = jnp.concatenate(
        [jnp.concatenate(factors, axis=1), line, jnp.zeros((SUB - 4, LANES), jnp.float32)],
        axis=0,
    )


def mark_kernel(value, out):
    out[...] = value[...]


def factor_kernel(own, par, xhi, xlo, *, geo, nblk, everywhere):
    piece = pieces_of(own, par, geo)
    devices = [(ix, iy) for ix in range(geo.gx) for iy in range(geo.gy)]
    size = own.shape[1] // (geo.nz if everywhere else 1)
    blocks = range(geo.nz if everywhere else 1)
    kept = (nblk + 1) // 2
    tops = geo.cy * nblk * geo.cz

    def top(zb, ix, k):
        side, pos = (1, k) if k < kept else (2, k - kept)
        return piece(ix, geo.gy - side, zb * size + tops + pos * geo.cz, geo.cz)

    for k in range(nblk):
        rows = [
            piece(ix, iy, zb * size + (slot * nblk + k) * geo.cz, geo.cz)
            for zb in blocks
            for ix, iy in devices
            for slot in range(geo.cy)
        ]
        for ix in range(geo.gx):
            for y in range(geo.wy):
                zb = geo.wy - 1 - y
                if zb in blocks:
                    rows.append(top(zb, ix, k))
                else:
                    rows.append(jnp.zeros((geo.cz, LANES), jnp.float32))
        high, rest = split(jnp.concatenate(rows, axis=0))
        xhi[k] = high
        xlo[k] = rest


def fine_kernel(
    own, par, eig, mref, tref, pref, res, inv, cur, resm, gref, labels, tmp, buf,
    *, geo, prow, everywhere
):
    piece = pieces_of(own, par, geo)
    devices = [(ix, iy) for ix in range(geo.gx) for iy in range(geo.gy)]
    per_chunk = LANES // geo.ne
    words = NF**3 // LANES
    for zb in range(geo.nz):
        for ch in range(geo.chunks):
            group = devices[ch * per_chunk : (ch + 1) * per_chunk]
            for blk in range(words):
                rows = [piece(ix, iy, zb * prow + blk * geo.ne, geo.ne) for ix, iy in group]
                square = jnp.concatenate(rows, axis=0)
                res[zb, ch, pl.ds(blk * LANES, LANES), :] = square.T
            total = None
            for pos, (ix, iy) in enumerate(group):
                part = piece(ix, iy, zb * prow + words * geo.ne, SUB)
                if everywhere or zb == geo.mid:
                    row = (zb if everywhere else 0) * geo.planes + ix * geo.gy + iy
                    labels[pl.ds(row, 1), :] = part[3:4]
                part = roll(part, pos * geo.ne)
                total = part if total is None else total + part
            gref[zb, ch] = total
    gather_sum(res, mref, geo, NF)
    local_diagonal(tmp, gref, tref, geo, FINE)
    gather_sum(tmp, mref, geo, NF)
    operate = functools.partial(apply_fine, gref=gref, tref=tref, pref=pref, geo=geo)
    first_smooth(res, inv, cur, tmp, mref, geo, FINE, scales(eig, 0), operate)
    restrict(res, tmp, resm, mref, tref, geo, NF, NM, UP_F, "rz8", buf)
    gather_sum(resm, mref, geo, NM)


def merge(src, dst, mref, geo):
    def body(pos):
        pos = pl.multiple_of(pos * SUB, SUB)
        for ch in range(geo.chunks):
            low_half = mref[NEXT_Z : NEXT_Z + 1, lane_ds(ch)] > 0.5
            row = pl.ds(pos, SUB)
            dst[0, ch, row, :] = src[geo.mid, ch, row, :]
            dst[1, ch, row, :] = jnp.where(
                low_half, src[geo.mid + 1, ch, row, :], src[geo.mid - 1, ch, row, :]
            )

    count = src.shape[2] // SUB
    lax.fori_loop(0, count, lambda pos, carry: (body(pos), carry)[1], 0, unroll=min(count, 16))


def middle_kernel(*refs, geo, everywhere):
    res, inv, cur, resm, gref, eig, mref, tref = refs[:8]
    merged, owned = refs[8:15], refs[15]
    invm, curm, tmpm, low, buf = refs[16:]
    local_diagonal(tmpm, gref, tref, geo, MID)
    gather_sum(tmpm, mref, geo, NM)
    operate = functools.partial(apply_middle, gref=gref, tref=tref, geo=geo)
    first_smooth(resm, invm, curm, tmpm, mref, geo, MID, scales(eig, 1), operate)
    restrict(resm, tmpm, low, mref, tref, geo, NM, NC, UP_C, "rz4", buf)
    z_lo = mref[MASK_Z_LO : MASK_Z_LO + 1, :] > 0.5
    y_lo = mref[MASK_Y_LO : MASK_Y_LO + 1, :]
    top = mref[TOP_ROW : TOP_ROW + 1, :]
    xs = geo.wy * geo.cz

    def node(zb, a, b, c):
        return wide_load(low, zb, pl.ds((a * NC + b) * SUB + c, 1), geo)

    def along_z(zb, a, b):
        before = roll(node((zb - 1) % geo.nz, a, b, 1), -(geo.cz - 1))
        return node(zb, a, b, 0) + jnp.where(z_lo, roll(node(zb, a, b, 1), 1), before)

    tops = None
    blocks = range(geo.nz) if everywhere else [geo.mid]
    for pos, zb in enumerate(blocks):
        grid = [[along_z(zb, a, b) for b in range(NC)] for a in range(NC)]
        floor = [grid[a][0] + y_lo * roll(grid[a][1], geo.cz) for a in range(NC)]
        owned[:, pl.ds(pos * geo.lanes, geo.lanes)] = jnp.broadcast_to(
            floor[0] + roll(floor[1], xs), (SUB, geo.lanes)
        )
        ceil = top * (grid[0][1] + roll(grid[1][1], xs))
        ceil = roll(ceil, -geo.cz * pos)
        tops = ceil if tops is None else tops + ceil
    owned[:, pl.ds(len(blocks) * geo.lanes, geo.lanes)] = jnp.broadcast_to(
        tops, (SUB, geo.lanes)
    )
    for source, target in zip((res, inv, cur, resm, invm, curm, gref), merged):
        merge(source, target, mref, geo)


def owner_mask(owners, count):
    width = owners.shape[1]
    row = lax.broadcasted_iota(jnp.int32, (count, width), 0)
    return jnp.broadcast_to(owners, (count, width)) == row


def contributions(owned, owners, xhi, xlo, nblk, count):
    spread = jnp.broadcast_to(owned[0:1, :], (count, owned.shape[1]))
    spread = jnp.where(owner_mask(owners, count), spread, 0.0)
    return [dot3(spread, xhi[k], xlo[k], ((1,), (0,))) for k in range(nblk)]


def pick_columns(values, labels, own_labels, nblk):
    count = own_labels.shape[0]
    every = labels.shape[0]
    id_rows = jnp.concatenate([own_labels[:, k : k + 1] for k in range(nblk)], axis=0)
    picked = None
    per_step = nblk if nblk * every <= 1024 else 1
    for k0 in range(0, nblk, per_step):
        ks = range(k0, k0 + per_step)
        cols = jnp.concatenate([labels[:, k : k + 1] for k in ks], axis=0)
        id_lanes = jnp.broadcast_to(cols, (cols.shape[0], LANES)).T[0:1]
        hit = (id_rows == id_lanes).astype(jnp.bfloat16)
        high, rest = split(jnp.concatenate([values[k] for k in ks], axis=0))
        part = dot(hit, high, ((1,), (0,))) + dot(hit, rest, ((1,), (0,)))
        picked = part if picked is None else picked + part
    return [picked[k * count : (k + 1) * count] for k in range(nblk)]


def solve_rows(picked, owners, xhi, xlo):
    full = None
    for k, value in enumerate(picked):
        part = dot3(value, xhi[k], xlo[k], ((1,), (1,)))
        full = part if full is None else full + part
    mine = owner_mask(owners, full.shape[0])
    return jnp.sum(jnp.where(mine, full, 0.0), axis=0, keepdims=True)


def send_kernel(owned, xhi, xlo, labels, send, *, geo, nblk):
    owners = geo.owners(False)
    for k, value in enumerate(contributions(owned, owners, xhi, xlo, nblk, geo.planes)):
        send[:, pl.ds(k * LANES, LANES)] = value
    send[:, pl.ds(nblk * LANES, LANES)] = labels[...]


def coarse_kernel(*refs, geo, nblk, peers):
    parts = refs[:peers]
    xhi, xlo, out = refs[peers:]
    owners = geo.owners(False)
    values = [
        jnp.concatenate([part[:, pl.ds(k * LANES, LANES)] for part in parts], axis=0)
        for k in range(nblk + 1)
    ]
    own_labels = parts[0][:, pl.ds(nblk * LANES, LANES)]
    picked = pick_columns(values[:nblk], values[nblk], own_labels, nblk)
    solved = solve_rows(picked, owners, xhi, xlo)
    out[pl.ds(0, 1), :] = solved[:, : geo.lanes]
    out[pl.ds(1, 1), :] = solved[:, geo.lanes :]


def rise(solved, state, consts, out, scratch, geo):
    res, inv, cur_in, resm, invm, curm_in, gref = state
    eig, mref, tref, pref = consts
    cur, curm, tmp, tmpm, step, stepm, low, turned = scratch
    y_hi = mref[MASK_Y_HI : MASK_Y_HI + 1, :] > 0.5
    z_hi = mref[MASK_Z_HI : MASK_Z_HI + 1, :] > 0.5
    xs = geo.wy * geo.cz
    levels = []
    for base, ceil in solved:
        upper = jnp.where(y_hi, roll(base, -geo.cz), ceil)
        flat = [base, upper]
        levels.append([flat, [roll(v, -xs) for v in flat]])
    low_half = mref[NEXT_Z : NEXT_Z + 1, :] > 0.5
    for a in range(NC):
        for b in range(NC):
            flat = [levels[zb][a][b] for zb in range(3)]
            deep = [
                jnp.where(z_hi, roll(flat[zb], -1), roll(flat[(zb + 1) % 3], geo.cz - 1))
                for zb in range(3)
            ]
            for c, value in enumerate((flat, deep)):
                row = pl.ds((a * NC + b) * SUB + c, 1)
                wide_store(low, 0, row, geo, value[1])
                wide_store(low, 1, row, geo, jnp.where(low_half, value[2], value[0]))
    prolong_add(low, curm_in, curm, tref, geo, NM, NC, UP_C, "pz4")
    operate = functools.partial(apply_middle, gref=gref, tref=tref, geo=geo)
    next_smooth(resm, invm, curm, stepm, tmpm, mref, geo, MID, scales(eig, 1), operate)
    prolong_add(curm, cur_in, cur, tref, geo, NF, NM, UP_F, "pz8")
    operate = functools.partial(apply_fine, gref=gref, tref=tref, pref=pref, geo=geo)
    next_smooth(res, inv, cur, step, tmp, mref, geo, FINE, scales(eig, 0), operate)
    words = NF**3 // LANES
    for ch in range(geo.chunks):
        for blk in range(words):
            turned[pl.ds(ch * LANES, LANES), pl.ds(blk * LANES, LANES)] = cur[
                geo.mid, ch, pl.ds(blk * LANES, LANES), :
            ].T
    my = lax.axis_index("gx") * geo.gy + lax.axis_index("gy")
    out[...] = turned[pl.ds(pl.multiple_of(my * geo.ne, SUB), geo.ne), :]


def up_kernel(*refs, geo):
    blocks = [(ref[0:1, :], ref[1:2, :]) for ref in refs[:3]]
    rest = refs[3:]
    rise(blocks, rest[:7], rest[7:11], rest[11], rest[12:], geo.window(2, 0))


def finish_kernel(owned, xhi, xlo, labels, *refs, geo, nblk):
    owners = geo.owners(True)
    values = contributions(owned, owners, xhi, xlo, nblk, labels.shape[0])
    names = labels[...]
    picked = pick_columns(values, names, names, nblk)
    solved = solve_rows(picked, owners, xhi, xlo)
    near = geo.window(2, 0)
    tops = solved[:, geo.nz * geo.lanes :]
    blocks = [
        (solved[:, zb * geo.lanes : (zb + 1) * geo.lanes], roll(tops, geo.cz * zb))
        for zb in range(3)
    ]
    rise(blocks, refs[:7], refs[7:11], refs[11], refs[12:], near)


def holds_all(gx, gy, gz, cy, cz):
    nodes = gx * gy * gz * cy * cz * NF**3
    return 3 <= gz <= gy * cy and nodes * 4 <= MAX_EVERYWHERE


def on_device(residual_in, geometry, eig_top, coarse_rows, block_ids, sizes, everywhere):
    gx, gy, gz = sizes
    cx, cy, cz = residual_in.shape[:3]
    nblk = coarse_rows.shape[3]
    geo = Geo(gx, gy, cy, cz, 3)
    if everywhere:
        geo = geo.window(gz)
    ok = cx == 1 and cz % SUB == 0 and LANES % geo.ne == 0 and geo.lanes % LANES == 0
    ok = ok and all(v & (v - 1) == 0 for v in (geo.ne, cz, geo.wy))
    if not ok or coarse_rows.shape[4] != LANES or geo.planes % SUB:
        raise ValueError("block shape")
    f32 = jnp.float32
    vmem = pl.BlockSpec(memory_space=pltpu.VMEM)
    smem = pl.BlockSpec(memory_space=pltpu.SMEM)
    half, cores = geo.half, geo.cores
    slots = (cy + 1) * cz
    prow = NF**3 // LANES * geo.ne + SUB

    def shape(dims, kind=f32):
        return jax.ShapeDtypeStruct(dims, kind)

    def call(body, specs, outs, scratch, *operands, extra=()):
        kept = list(operands) + list(outs) + list(scratch)
        total = sum(math.prod(a.shape) * a.dtype.itemsize for a in kept)
        return pl.pallas_call(
            body,
            out_shape=list(outs),
            in_specs=specs,
            out_specs=[vmem] * len(outs),
            scratch_shapes=[pltpu.VMEM(a.shape, a.dtype) for a in scratch] + list(extra),
            compiler_params=pltpu.CompilerParams(
                vmem_limit_bytes=min(total + (3 << 20), 60 << 20)
            ),
        )(*operands)

    def rank(ix, ih, core):
        return (ix % gx) * gy + (ih % half) * cores + core

    def across_chips(value):
        parts = [value]
        for dx in range(gx):
            for dh in range(half):
                if dx or dh:
                    pairs = [
                        (rank(ix + dx, ih + dh, core), rank(ix, ih, core))
                        for ix in range(gx)
                        for ih in range(half)
                        for core in range(cores)
                    ]
                    parts.append(lax.ppermute(value, ("gx", "gy"), pairs))
        return parts

    def between_cores(value):
        if cores == 1:
            return value
        return lax.ppermute(value, "gy", [(i, i ^ 1) for i in range(gy)])

    hbm = pl.BlockSpec(memory_space=pltpu.HBM)
    factor = coarse_rows.reshape(cy + 1, cz, nblk, LANES).transpose(0, 2, 1, 3)
    part = shape(((nblk + 1) // 2 * cz, LANES))
    block, factor, keep, give, scale = call(
        functools.partial(pack_kernel, geo=geo),
        [hbm] * 5,
        [shape((prow, LANES)), shape((cy * nblk * cz, LANES)), part, part, shape((SUB, LANES))],
        [shape(geometry.shape), jax.ShapeDtypeStruct(block_ids.shape, block_ids.dtype)],
        *[
            pltpu.with_memory_space_constraint(value, pltpu.HBM)
            for value in (
                residual_in.reshape(geo.ne, NF**3),
                geometry,
                factor.reshape(slots * nblk, LANES),
                block_ids,
                eig_top,
            )
        ],
        extra=[pltpu.SMEM((2,), f32), pltpu.SemaphoreType.DMA((NF**3 // LANES + 6,))],
    )
    marks = [call(mark_kernel, [vmem], [shape((SUB, LANES))], [], scale)[0] for _ in range(2)]

    def from_block(value, offset):
        return lax.ppermute(value, "gz", [((i + offset) % gz, i) for i in range(gz)])

    def along_z(value):
        order = list(range(2, geo.nz - 1)) + [-1, 1]
        got = {offset: from_block(value, offset) for offset in order}
        got[0] = value
        return jnp.concatenate([got[offset] for offset in sorted(got)], axis=0)

    taken = lax.ppermute(give, "gy", [(gy - 1, gy - 2)])
    keep = jnp.where(lax.axis_index("gy") == gy - 1, keep, taken)
    factor = jnp.concatenate([factor, keep], axis=0)
    column = along_z(block)
    if everywhere:
        factor = along_z(factor)
    own = jnp.stack(across_chips(column))
    par = between_cores(own)
    factor_own = across_chips(factor)

    masks = jnp.asarray(geo.masks())
    table = jnp.asarray(TABLE)
    planes = jnp.asarray(PLANES)
    count = geo.planes * (geo.nz if everywhere else 1)
    width = ((geo.nz if everywhere else 1) + 1) * geo.lanes
    near = geo.window(2, 0)

    def field(where, points):
        return shape((where.nz, where.chunks, points * points * SUB, LANES))

    fine, middle, lowest = (field(geo, points) for points in (NF, NM, NC))
    buf = shape((1, 1, NM * NM * SUB, LANES))
    metric = shape((geo.nz, geo.chunks, SUB, LANES))
    res, inv, cur, resm, gfac, names = call(
        functools.partial(fine_kernel, geo=geo, prow=prow, everywhere=everywhere),
        [vmem] * 6,
        [fine] * 3 + [middle, metric, shape((count, LANES))],
        [fine, buf],
        own, par, marks[1], masks, table, planes,
    )
    factor_par = jnp.stack([between_cores(part) for part in factor_own])
    factor_own = jnp.stack(factor_own)
    fine2, middle2 = (field(near, points) for points in (NF, NM))
    *merged, owned = call(
        functools.partial(middle_kernel, geo=geo, everywhere=everywhere),
        [vmem] * 8,
        [fine2] * 3
        + [middle2] * 3
        + [shape((2, geo.chunks, SUB, LANES)), shape((SUB, width))],
        [middle, middle, middle, lowest, buf],
        res, inv, cur, resm, gfac, marks[0], masks, table,
    )
    wide = shape((nblk, width, LANES), jnp.bfloat16)
    xhi, xlo = call(
        functools.partial(factor_kernel, geo=geo, nblk=nblk, everywhere=everywhere),
        [vmem, vmem],
        [wide, wide],
        [],
        factor_own, factor_par,
    )
    state = (*merged, scale, masks, table, planes)
    kinds = [vmem] * 11
    final = shape((geo.ne, NF**3))
    scratch = [fine2, middle2] * 3 + [field(near, NC), shape((geo.lanes, NF**3))]
    if everywhere:
        (out,) = call(
            functools.partial(finish_kernel, geo=geo, nblk=nblk),
            [vmem] * 4 + kinds,
            [final],
            scratch,
            owned, xhi, xlo, names, *state,
        )
        return out.reshape(cx, cy, cz, NF**3)

    (send,) = call(
        functools.partial(send_kernel, geo=geo, nblk=nblk),
        [vmem] * 4,
        [shape((geo.planes, (nblk + 1) * LANES))],
        [],
        owned, xhi, xlo, names,
    )
    parts = [send] + [from_block(send, offset) for offset in range(1, gz)]
    (solved,) = call(
        functools.partial(coarse_kernel, geo=geo, nblk=nblk, peers=gz),
        [vmem] * (gz + 2),
        [shape((SUB, geo.lanes))],
        [],
        *parts, xhi, xlo,
    )
    (out,) = call(
        functools.partial(up_kernel, geo=geo),
        [vmem] * 3 + kinds,
        [final],
        scratch,
        from_block(solved, -1), solved, from_block(solved, 1), *state,
    )
    return out.reshape(cx, cy, cz, NF**3)


def solution(mesh):
    sizes = tuple(mesh.shape[name] for name in ("gx", "gy", "gz"))
    in_specs = (
        P("gx", "gy", "gz", None),
        P(None, "gx", "gy", "gz"),
        P(),
        P("gx", "gy", "gz", None, None),
        P("gx", "gy", "gz", None),
    )
    out_specs = P("gx", "gy", "gz", None)

    def program(residual_in, geometry, eig_top, coarse_rows, block_ids):
        gx, gy, gz = sizes
        cy, cz = residual_in.shape[1] // gy, residual_in.shape[2] // gz
        everywhere = holds_all(gx, gy, gz, cy, cz)

        def body(*blocks):
            return on_device(*blocks, sizes=sizes, everywhere=everywhere)

        step = jax.shard_map(
            body, mesh=mesh, in_specs=in_specs, out_specs=out_specs, check_vma=False
        )
        return step(residual_in, geometry, eig_top, coarse_rows, block_ids)

    return program
```

```python
import functools
import math

import jax
import jax.numpy as jnp
import numpy as np
from jax import lax
from jax.experimental import pallas as pl
from jax.experimental.pallas import tpu as pltpu
from jax.sharding import PartitionSpec as P


NF = 8
NM = 4
NC = 2
LANES = 128
SUB = 8
MAX_EVERYWHERE = 2 << 20
SIGMA = 0.55 / 0.45
RHO0 = 1.0 / SIGMA
RHO1 = 1.0 / (2.0 * SIGMA - RHO0)


def legendre_pair(point, degree):
    previous = 1.0
    current = point
    for order in range(1, degree):
        following = ((2 * order + 1) * point * current - order * previous) / (order + 1)
        previous = current
        current = following
    return (current, previous)


def gll_tables(points):
    degree = points - 1
    node_list = []
    for index in range(points):
        guess = -math.cos(math.pi * index / degree)
        for _ in range(100):
            high_val, low_val = legendre_pair(guess, degree)
            guess = guess - (guess * high_val - low_val) / (points * high_val)
        node_list.append(guess)
    node_list[0] = -1.0
    node_list[degree] = 1.0
    node_pos = np.array(node_list)
    at_nodes = np.array([legendre_pair(value, degree)[0] for value in node_list])
    weights = 2.0 / (degree * (degree + 1) * at_nodes**2)
    derivative = np.zeros((points, points))
    for row_pos in range(points):
        for col_pos in range(points):
            if row_pos != col_pos:
                derivative[row_pos, col_pos] = at_nodes[row_pos] / (
                    at_nodes[col_pos] * (node_pos[row_pos] - node_pos[col_pos])
                )
    derivative[0, 0] = -degree * (degree + 1) / 4.0
    derivative[degree, degree] = degree * (degree + 1) / 4.0
    stiffness = derivative.T @ (weights[:, None] * derivative)
    return (node_pos, weights, stiffness)


def interp_table(fine_pts, coarse_pts):
    fine_nodes = gll_tables(fine_pts)[0]
    coarse_nodes = gll_tables(coarse_pts)[0]
    lagrange = np.ones((fine_pts, coarse_pts))
    for col_pos in range(coarse_pts):
        for other_pos in range(coarse_pts):
            if other_pos != col_pos:
                lagrange[:, col_pos] *= (fine_nodes - coarse_nodes[other_pos]) / (
                    coarse_nodes[col_pos] - coarse_nodes[other_pos]
                )
    return lagrange


class Level:
    def __init__(self, points):
        self.n = points
        _, weights, stiffness = gll_tables(points)
        self.w = [float(v) for v in weights]
        self.kd = [float(v) for v in np.diag(stiffness)]
        scaled = stiffness / weights[:, None]
        half = points // 2
        flipped = scaled[:, ::-1]
        self.even = [[float(v) for v in row[:half]] for row in (scaled + flipped)[:half] / 2]
        self.odd = [[float(v) for v in row[:half]] for row in (scaled - flipped)[:half] / 2]
        self.scaled = scaled
        self.weights = weights
        self.diag = np.diag(stiffness)


FINE = Level(NF)
MID = Level(NM)
UP_F = interp_table(NF, NM)
UP_C = interp_table(NM, NC)


def shared_faces(lagrange):
    out = lagrange.copy()
    out[0] *= 0.5
    out[-1] *= 0.5
    return out


def pad_rows(column, fill=0.0):
    out = np.full((SUB,), fill)
    out[: column.shape[0]] = column
    return out


def build_tables():
    rows = []
    index = {}

    def put(name, columns):
        index[name] = len(rows)
        rows.extend(columns)

    put("kz8", [FINE.scaled[:, c] for c in range(NF)])
    put("kz4", [pad_rows(MID.scaled[:, c]) for c in range(NM)])
    put("w8", [FINE.weights])
    put("w4", [pad_rows(MID.weights, 1.0)])
    put("kd8", [FINE.diag])
    put("kd4", [pad_rows(MID.diag, 1.0)])
    put("rz8", [pad_rows(shared_faces(UP_F)[c]) for c in range(NF)])
    put("rz4", [pad_rows(shared_faces(UP_C)[c]) for c in range(NM)])
    put("pz8", [UP_F[:, c] for c in range(NM)])
    put("pz4", [pad_rows(UP_C[:, c]) for c in range(NC)])
    flat = np.concatenate(rows).astype(np.float32)
    return np.ascontiguousarray(np.broadcast_to(flat[:, None], (flat.shape[0], LANES))), index


TABLE, TINDEX = build_tables()


def plane_products(level):
    weight = np.diag(level.weights)
    stiff = level.weights[:, None] * level.scaled
    both = np.concatenate([np.kron(stiff, weight), np.kron(weight, stiff)], axis=0)
    both = both.astype(np.float32)
    high = both.astype(jnp.bfloat16)
    low = (both - high.astype(np.float32)).astype(jnp.bfloat16)
    return np.concatenate([high, high, low, low], axis=1)


PLANES = plane_products(FINE)
MASK_Y_LO, MASK_Y_HI, MASK_Z_LO, MASK_Z_HI, FAC_Y_LO, FAC_Y_HI, TOP_ROW, NEXT_Z = range(8)


class Geo:
    def __init__(self, gx, gy, cy, cz, nz):
        self.gx, self.gy, self.cy, self.cz, self.nz = gx, gy, cy, cz, nz
        self.wy = gy * cy
        self.lanes = gx * self.wy * cz
        self.ne = cy * cz
        self.planes = gx * gy
        self.half = gy // 2 if gy % 2 == 0 else gy
        self.cores = gy // self.half
        self.chunks = self.lanes // LANES
        self.mid = 1

    def window(self, nz, mid=1):
        out = Geo(self.gx, self.gy, self.cy, self.cz, nz)
        out.mid = mid
        return out

    def owners(self, everywhere):
        blocks = self.nz if everywhere else 1
        width = (blocks + 1) * self.lanes
        place = lax.broadcasted_iota(jnp.int32, (1, width), 1)
        base = lax.shift_right_logical(place, self.ne.bit_length() - 1)
        rest = place - blocks * self.lanes
        y = lax.shift_right_logical(rest, self.cz.bit_length() - 1) & (self.wy - 1)
        x = lax.shift_right_logical(rest, (self.cz * self.wy).bit_length() - 1)
        zb = self.wy - 1 - y
        top = jnp.where(zb < blocks, zb * self.planes + x * self.gy + self.gy - 1, -1)
        return jnp.where(rest < 0, base, top)

    def masks(self):
        lane = np.arange(self.lanes)
        z = lane % self.cz
        y = (lane // self.cz) % self.wy
        out = np.zeros((8, self.lanes), np.float32)
        out[MASK_Y_LO] = y > 0
        out[MASK_Y_HI] = y < self.wy - 1
        out[MASK_Z_LO] = z > 0
        out[MASK_Z_HI] = z < self.cz - 1
        out[FAC_Y_LO] = np.where(y > 0, 0.5, 1.0)
        out[FAC_Y_HI] = np.where(y < self.wy - 1, 0.5, 1.0)
        out[TOP_ROW] = y == self.wy - 1
        out[NEXT_Z] = z < self.cz // 2
        return out


def roll(value, shift):
    size = value.shape[-1]
    shift %= size
    return value if shift == 0 else pltpu.roll(value, shift, axis=value.ndim - 1)


def tab(tref, name, pos=0):
    return tref[pl.ds((TINDEX[name] + pos) * SUB, SUB), :]


def lane_ds(chunk):
    if isinstance(chunk, int):
        return pl.ds(chunk * LANES, LANES)
    return pl.ds(pl.multiple_of(chunk * LANES, LANES), LANES)


def for_tiles(geo, body, unroll=1):
    def step(pos, carry):
        if geo.chunks == 1:
            body(pos, 0)
        else:
            body(pos // geo.chunks, pos % geo.chunks)
        return carry

    lax.fori_loop(0, geo.nz * geo.chunks, step, 0, unroll=unroll)


def rows8(pos):
    if isinstance(pos, int):
        return pl.ds(pos * SUB, SUB)
    return pl.ds(pl.multiple_of(pos * SUB, SUB), SUB)


def wide_load(ref, zb, rows, geo):
    parts = [ref[zb, ch, rows, :] for ch in range(geo.chunks)]
    return parts[0] if len(parts) == 1 else jnp.concatenate(parts, axis=1)


def wide_store(ref, zb, rows, geo, value):
    for ch in range(geo.chunks):
        ref[zb, ch, rows, :] = value[:, ch * LANES : (ch + 1) * LANES]


def gather_sum(ref, mref, geo, n):
    xs = geo.wy * geo.cz
    last = (n - 1) * n
    for b in range(n):
        for zb in range(geo.nz):
            low = wide_load(ref, zb, rows8(b), geo)
            high = wide_load(ref, zb, rows8(last + b), geo)
            wide_store(ref, zb, rows8(b), geo, low + roll(high, xs))
            wide_store(ref, zb, rows8(last + b), geo, high + roll(low, -xs))
    y_lo = mref[MASK_Y_LO : MASK_Y_LO + 1, :]
    y_hi = mref[MASK_Y_HI : MASK_Y_HI + 1, :]
    for a in range(n):
        first, final = rows8(a * n), rows8(a * n + n - 1)
        for zb in range(geo.nz):
            low = wide_load(ref, zb, first, geo)
            high = wide_load(ref, zb, final, geo)
            wide_store(ref, zb, first, geo, low + y_lo * roll(high, geo.cz))
            wide_store(ref, zb, final, geo, high + y_hi * roll(low, -geo.cz))
    z_lo = mref[MASK_Z_LO : MASK_Z_LO + 1, :] > 0.5
    z_hi = mref[MASK_Z_HI : MASK_Z_HI + 1, :] > 0.5
    group = min(SUB, n * n)
    for g in range(n * n // group):
        first = pl.ds(g * group * SUB, group, stride=SUB)
        final = pl.ds(g * group * SUB + n - 1, group, stride=SUB)
        low = [wide_load(ref, zb, first, geo) for zb in range(geo.nz)]
        high = [wide_load(ref, zb, final, geo) for zb in range(geo.nz)]
        for zb in range(geo.nz):
            before = roll(high[(zb - 1) % geo.nz], -(geo.cz - 1))
            after = roll(low[(zb + 1) % geo.nz], geo.cz - 1)
            near = jnp.where(z_lo, roll(high[zb], 1), before)
            wide_store(ref, zb, first, geo, low[zb] + near)
            near = jnp.where(z_hi, roll(low[zb], -1), after)
            wide_store(ref, zb, final, geo, high[zb] + near)


def contract(values, level):
    half = level.n // 2
    sums = [values[a] + values[level.n - 1 - a] for a in range(half)]
    diffs = [values[a] - values[level.n - 1 - a] for a in range(half)]
    out = [None] * level.n
    for i in range(half):
        even = sums[0] * level.even[i][0]
        odd = diffs[0] * level.odd[i][0]
        for a in range(1, half):
            even = even + sums[a] * level.even[i][a]
            odd = odd + diffs[a] * level.odd[i][a]
        out[i] = even + odd
        out[level.n - 1 - i] = even - odd
    return out


def combine(values, table):
    out = []
    for i in range(table.shape[0]):
        total = values[0] * float(table[i, 0])
        for a in range(1, table.shape[1]):
            total = total + values[a] * float(table[i, a])
        out.append(total)
    return out


def sublane_mix(ref, zb, ch, row, columns):
    total = ref[zb, ch, pl.ds(row, 1), :] * columns[0]
    for c in range(1, len(columns)):
        total = total + ref[zb, ch, pl.ds(row + c, 1), :] * columns[c]
    return total


def apply_fine(src, dst, gref, tref, pref, geo):
    level = FINE
    n = level.n

    def body(zb, ch):
        wc = tab(tref, "w8")
        g0, g1, g2 = [gref[zb, ch, pl.ds(i, 1), :] for i in range(3)]
        gw = g0 * wc
        for b in range(n):
            mixed = contract([src[zb, ch, rows8(a * n + b), :] for a in range(n)], level)
            factors = [gw * (level.w[b] * level.w[a]) for a in range(n // 2)]
            for a in range(n):
                dst[zb, ch, rows8(a * n + b), :] = mixed[a] * factors[min(a, n - 1 - a)]
        planes = pref[...]
        for a in range(n):
            slab = pl.ds(a * n * SUB, n * SUB)
            high, low = split(src[zb, ch, slab, :])
            data = jnp.concatenate([high, low, high, low], axis=0)
            both = dot(planes, data, ((1,), (0,)))
            total = both[: n * SUB] * g1 + both[n * SUB :] * g2
            dst[zb, ch, slab, :] = dst[zb, ch, slab, :] + total * level.w[a]

    for_tiles(geo, body, unroll=2 if geo.nz * geo.chunks > 2 else 1)


def apply_middle(src, dst, gref, tref, geo):
    level = MID
    n = level.n
    kname, wname = "kz4", "w4"

    def body(zb, ch):
        ln = lane_ds(ch)
        wc = tab(tref, wname)
        gw = [gref[zb, ch, pl.ds(i, 1), :] * wc for i in range(3)]
        columns = [tab(tref, kname, c) for c in range(n)]
        for b in range(n):
            mixed = contract([src[zb, ch, rows8(a * n + b), :] for a in range(n)], level)
            for a in range(n):
                dst[zb, ch, rows8(a * n + b), :] = mixed[a] * gw[0]
        for a in range(n):
            mixed = contract([src[zb, ch, rows8(a * n + b), :] for b in range(n)], level)
            for b in range(n):
                row = (a * n + b) * SUB
                along = sublane_mix(src, zb, ch, row, columns)
                total = dst[zb, ch, rows8(a * n + b), :] + mixed[b] * gw[1] + along * gw[2]
                dst[zb, ch, rows8(a * n + b), :] = total * (level.w[a] * level.w[b])

    for_tiles(geo, body)


def local_diagonal(dst, gref, tref, geo, level):
    n = level.n
    wname, dname = ("w8", "kd8") if n == NF else ("w4", "kd4")

    def body(zb, ch):
        ln = lane_ds(ch)
        wc = tab(tref, wname)
        gx = gref[zb, ch, pl.ds(0, 1), :] * wc
        gy = gref[zb, ch, pl.ds(1, 1), :] * wc
        gz = gref[zb, ch, pl.ds(2, 1), :] * tab(tref, dname)
        for a in range(n):
            for b in range(n):
                dst[zb, ch, rows8(a * n + b), :] = (
                    gx * (level.kd[a] * level.w[b])
                    + gy * (level.w[a] * level.kd[b])
                    + gz * (level.w[a] * level.w[b])
                )

    for_tiles(geo, body)


def each_row(geo, n, body, blocks=None):
    def tile(zb, ch):
        for row in range(n * n):
            body(zb, ch, rows8(row))

    for_tiles(geo if blocks is None else geo.window(blocks), tile)


def scales(ref, level):
    return ref[2 * level : 2 * level + 1, :], ref[2 * level + 1 : 2 * level + 2, :]


def first_smooth(res, inv, cur, tmp, mref, geo, level, top, operate):
    first, second = top

    def start(zb, ch, row):
        value = 1.0 / tmp[zb, ch, row, :]
        inv[zb, ch, row, :] = value
        cur[zb, ch, row, :] = value * res[zb, ch, row, :] * first

    each_row(geo, level.n, start)
    operate(cur, tmp)
    gather_sum(tmp, mref, geo, level.n)

    def finish(zb, ch, row):
        left = res[zb, ch, row, :] - tmp[zb, ch, row, :]
        cur[zb, ch, row, :] = (1.0 + RHO0 * RHO1) * cur[zb, ch, row, :] + second * (
            inv[zb, ch, row, :] * left
        )

    each_row(geo, level.n, finish)
    operate(cur, tmp)
    gather_sum(tmp, mref, geo, level.n)


def next_smooth(res, inv, cur, step, tmp, mref, geo, level, top, operate):
    first, second = top
    operate(cur, tmp)
    gather_sum(tmp, mref, geo, level.n)

    def start(zb, ch, row):
        value = inv[zb, ch, row, :] * (res[zb, ch, row, :] - tmp[zb, ch, row, :]) * first
        step[zb, ch, row, :] = value
        cur[zb, ch, row, :] = cur[zb, ch, row, :] + value

    each_row(geo, level.n, start)
    operate(cur, tmp)
    gather_sum(tmp, mref, geo, level.n)

    def finish(zb, ch, row):
        left = res[zb, ch, row, :] - tmp[zb, ch, row, :]
        cur[zb, ch, row, :] = (
            cur[zb, ch, row, :]
            + (RHO0 * RHO1) * step[zb, ch, row, :]
            + second * (inv[zb, ch, row, :] * left)
        )

    each_row(geo, level.n, finish, 1 if level.n == NF else None)


def restrict(res, tmp, dst, mref, tref, geo, nf, nc, table, name, buf):
    scaled = shared_faces(table)

    def body(zb, ch):
        ln = lane_ds(ch)
        f_lo = mref[FAC_Y_LO : FAC_Y_LO + 1, ln]
        f_hi = mref[FAC_Y_HI : FAC_Y_HI + 1, ln]
        part = []
        for b in range(nf):
            values = []
            for a in range(nf):
                row = rows8(a * nf + b)
                values.append(res[zb, ch, row, :] - tmp[zb, ch, row, :])
            mixed = combine(values, scaled.T)
            if b == 0:
                mixed = [v * f_lo for v in mixed]
            if b == nf - 1:
                mixed = [v * f_hi for v in mixed]
            part.append(mixed)
        columns = [tab(tref, name, c) for c in range(nf)]
        for i in range(nc):
            along = combine([part[b][i] for b in range(nf)], table.T)
            for j in range(nc):
                buf[0, 0, rows8(i * nc + j), :] = along[j]
        for row in range(nc * nc):
            dst[zb, ch, rows8(row), :] = sublane_mix(buf, 0, 0, row * SUB, columns)

    for_tiles(geo, body)


def prolong_add(src, base, cur, tref, geo, nf, nc, table, name):
    def body(zb, ch):
        ln = lane_ds(ch)
        columns = [tab(tref, name, c) for c in range(nc)]
        part = []
        for a in range(nc):
            deep = [
                sublane_mix(src, zb, ch, (a * nc + b) * SUB, columns) for b in range(nc)
            ]
            part.append(combine(deep, table))
        for b in range(nf):
            mixed = combine([part[a][b] for a in range(nc)], table)
            for a in range(nf):
                row = rows8(a * nf + b)
                cur[zb, ch, row, :] = base[zb, ch, row, :] + mixed[a]

    for_tiles(geo, body)


def split(value):
    high = value.astype(jnp.bfloat16)
    return high, (value - high.astype(jnp.float32)).astype(jnp.bfloat16)


def dot(left, right, dims):
    return lax.dot_general(left, right, (dims, ((), ())), preferred_element_type=jnp.float32)


def dot3(left, right_high, right_low, dims):
    high, low = split(left)
    return dot(high, right_high, dims) + (dot(high, right_low, dims) + dot(low, right_high, dims))


def pieces_of(own, par, geo):
    my_x = lax.axis_index("gx")
    my_y = lax.axis_index("gy")
    my_h = my_y // geo.cores
    my_c = my_y % geo.cores

    def piece(ix, iy, start, size):
        rel = lax.rem(ix - my_x + geo.gx, geo.gx) * geo.half + lax.rem(
            iy // geo.cores - my_h + geo.half, geo.half
        )
        mine = own[rel, pl.ds(start, size), :]
        if geo.cores == 1:
            return mine
        return jnp.where(my_c == iy % geo.cores, mine, par[rel, pl.ds(start, size), :])

    return piece


def pack_kernel(
    residual, geometry, factor, ids, eig, block, rows, keep, give, scale, metric, names, tops,
    sems, *, geo,
):
    words = NF**3 // LANES
    nblk = ids.shape[-1]
    base, kept, given = rows.shape[0], keep.shape[0], nblk * geo.cz - keep.shape[0]
    pieces = [
        (
            residual.at[:, pl.ds(blk * LANES, LANES)],
            block.at[pl.ds(blk * geo.ne, geo.ne), :],
        )
        for blk in range(words)
    ]
    pieces += [
        (geometry, metric),
        (ids, names),
        (eig, tops),
        (factor.at[pl.ds(0, base), :], rows),
        (factor.at[pl.ds(base, kept), :], keep),
        (factor.at[pl.ds(base + kept, given), :], give.at[pl.ds(0, given), :]),
    ]
    copies = [
        pltpu.make_async_copy(source, target, sems.at[pos])
        for pos, (source, target) in enumerate(pieces)
    ]
    for copy in copies:
        copy.start()
    if given < kept:
        give[pl.ds(given, kept - given), :] = jnp.zeros((kept - given, LANES), jnp.float32)
    for copy in copies:
        copy.wait()
    lines = []
    for level in range(2):
        lines.append(jnp.full((1, LANES), 1.0 / (0.55 * tops[level]), jnp.float32))
        lines.append(jnp.full((1, LANES), 2.0 * RHO1 / (0.45 * tops[level]), jnp.float32))
    lines.append(jnp.zeros((SUB - 4, LANES), jnp.float32))
    scale[...] = jnp.concatenate(lines, axis=0)
    factors = [metric[:, 0, y, :] for y in range(geo.cy)]
    factors.append(jnp.zeros((3, LANES - geo.ne), jnp.float32))
    line = names[0, 0].astype(jnp.float32)
    line = jnp.concatenate([line, jnp.zeros((1, LANES - nblk), jnp.float32)], axis=1)
    block[pl.ds(words * geo.ne, SUB), :] = jnp.concatenate(
        [jnp.concatenate(factors, axis=1), line, jnp.zeros((SUB - 4, LANES), jnp.float32)],
        axis=0,
    )


def mark_kernel(value, out):
    out[...] = value[...]


def factor_kernel(own, par, xhi, xlo, *, geo, nblk, everywhere):
    piece = pieces_of(own, par, geo)
    devices = [(ix, iy) for ix in range(geo.gx) for iy in range(geo.gy)]
    size = own.shape[1] // (geo.nz if everywhere else 1)
    blocks = range(geo.nz if everywhere else 1)
    kept = (nblk + 1) // 2
    tops = geo.cy * nblk * geo.cz

    def top(zb, ix, k):
        side, pos = (1, k) if k < kept else (2, k - kept)
        return piece(ix, geo.gy - side, zb * size + tops + pos * geo.cz, geo.cz)

    for k in range(nblk):
        rows = [
            piece(ix, iy, zb * size + (slot * nblk + k) * geo.cz, geo.cz)
            for zb in blocks
            for ix, iy in devices
            for slot in range(geo.cy)
        ]
        for ix in range(geo.gx):
            for y in range(geo.wy):
                zb = geo.wy - 1 - y
                if zb in blocks:
                    rows.append(top(zb, ix, k))
                else:
                    rows.append(jnp.zeros((geo.cz, LANES), jnp.float32))
        high, rest = split(jnp.concatenate(rows, axis=0))
        xhi[k] = high
        xlo[k] = rest


def fine_kernel(
    own, par, eig, mref, tref, pref, res2, inv2, cur2, resm, gref, labels,
    res, inv, cur, tmp, buf,
    *, geo, prow, everywhere
):
    piece = pieces_of(own, par, geo)
    devices = [(ix, iy) for ix in range(geo.gx) for iy in range(geo.gy)]
    per_chunk = LANES // geo.ne
    words = NF**3 // LANES
    for zb in range(geo.nz):
        for ch in range(geo.chunks):
            group = devices[ch * per_chunk : (ch + 1) * per_chunk]
            for blk in range(words):
                rows = [piece(ix, iy, zb * prow + blk * geo.ne, geo.ne) for ix, iy in group]
                square = jnp.concatenate(rows, axis=0)
                res[zb, ch, pl.ds(blk * LANES, LANES), :] = square.T
            total = None
            for pos, (ix, iy) in enumerate(group):
                part = piece(ix, iy, zb * prow + words * geo.ne, SUB)
                if everywhere or zb == geo.mid:
                    row = (zb if everywhere else 0) * geo.planes + ix * geo.gy + iy
                    labels[pl.ds(row, 1), :] = part[3:4]
                part = roll(part, pos * geo.ne)
                total = part if total is None else total + part
            gref[zb, ch] = total
    gather_sum(res, mref, geo, NF)
    local_diagonal(tmp, gref, tref, geo, FINE)
    gather_sum(tmp, mref, geo, NF)
    operate = functools.partial(apply_fine, gref=gref, tref=tref, pref=pref, geo=geo)
    first_smooth(res, inv, cur, tmp, mref, geo, FINE, scales(eig, 0), operate)
    restrict(res, tmp, resm, mref, tref, geo, NF, NM, UP_F, "rz8", buf)
    gather_sum(resm, mref, geo, NM)
    for source, target in zip((res, inv, cur), (res2, inv2, cur2)):
        merge(source, target, mref, geo)


def merge(src, dst, mref, geo):
    def body(pos):
        pos = pl.multiple_of(pos * SUB, SUB)
        for ch in range(geo.chunks):
            low_half = mref[NEXT_Z : NEXT_Z + 1, lane_ds(ch)] > 0.5
            row = pl.ds(pos, SUB)
            dst[0, ch, row, :] = src[geo.mid, ch, row, :]
            dst[1, ch, row, :] = jnp.where(
                low_half, src[geo.mid + 1, ch, row, :], src[geo.mid - 1, ch, row, :]
            )

    count = src.shape[2] // SUB
    lax.fori_loop(0, count, lambda pos, carry: (body(pos), carry)[1], 0, unroll=min(count, 16))


def middle_kernel(*refs, geo, everywhere):
    resm, gref, eig, mref, tref = refs[:5]
    merged, owned = refs[5:9], refs[9]
    invm, curm, tmpm, low, buf = refs[10:]
    local_diagonal(tmpm, gref, tref, geo, MID)
    gather_sum(tmpm, mref, geo, NM)
    operate = functools.partial(apply_middle, gref=gref, tref=tref, geo=geo)
    first_smooth(resm, invm, curm, tmpm, mref, geo, MID, scales(eig, 1), operate)
    restrict(resm, tmpm, low, mref, tref, geo, NM, NC, UP_C, "rz4", buf)
    z_lo = mref[MASK_Z_LO : MASK_Z_LO + 1, :] > 0.5
    y_lo = mref[MASK_Y_LO : MASK_Y_LO + 1, :]
    top = mref[TOP_ROW : TOP_ROW + 1, :]
    xs = geo.wy * geo.cz

    def node(zb, a, b, c):
        return wide_load(low, zb, pl.ds((a * NC + b) * SUB + c, 1), geo)

    def along_z(zb, a, b):
        before = roll(node((zb - 1) % geo.nz, a, b, 1), -(geo.cz - 1))
        return node(zb, a, b, 0) + jnp.where(z_lo, roll(node(zb, a, b, 1), 1), before)

    tops = None
    blocks = range(geo.nz) if everywhere else [geo.mid]
    for pos, zb in enumerate(blocks):
        grid = [[along_z(zb, a, b) for b in range(NC)] for a in range(NC)]
        floor = [grid[a][0] + y_lo * roll(grid[a][1], geo.cz) for a in range(NC)]
        owned[:, pl.ds(pos * geo.lanes, geo.lanes)] = jnp.broadcast_to(
            floor[0] + roll(floor[1], xs), (SUB, geo.lanes)
        )
        ceil = top * (grid[0][1] + roll(grid[1][1], xs))
        ceil = roll(ceil, -geo.cz * pos)
        tops = ceil if tops is None else tops + ceil
    owned[:, pl.ds(len(blocks) * geo.lanes, geo.lanes)] = jnp.broadcast_to(
        tops, (SUB, geo.lanes)
    )
    for source, target in zip((resm, invm, curm, gref), merged):
        merge(source, target, mref, geo)


def owner_mask(owners, count):
    width = owners.shape[1]
    row = lax.broadcasted_iota(jnp.int32, (count, width), 0)
    return jnp.broadcast_to(owners, (count, width)) == row


def contributions(owned, owners, xhi, xlo, nblk, count):
    spread = jnp.broadcast_to(owned[0:1, :], (count, owned.shape[1]))
    spread = jnp.where(owner_mask(owners, count), spread, 0.0)
    return [dot3(spread, xhi[k], xlo[k], ((1,), (0,))) for k in range(nblk)]


def pick_columns(values, labels, own_labels, nblk):
    count = own_labels.shape[0]
    every = labels.shape[0]
    id_rows = jnp.concatenate([own_labels[:, k : k + 1] for k in range(nblk)], axis=0)
    picked = None
    per_step = nblk if nblk * every <= 1024 else 1
    for k0 in range(0, nblk, per_step):
        ks = range(k0, k0 + per_step)
        cols = jnp.concatenate([labels[:, k : k + 1] for k in ks], axis=0)
        id_lanes = jnp.broadcast_to(cols, (cols.shape[0], LANES)).T[0:1]
        hit = (id_rows == id_lanes).astype(jnp.bfloat16)
        high, rest = split(jnp.concatenate([values[k] for k in ks], axis=0))
        part = dot(hit, high, ((1,), (0,))) + dot(hit, rest, ((1,), (0,)))
        picked = part if picked is None else picked + part
    return [picked[k * count : (k + 1) * count] for k in range(nblk)]


def solve_rows(picked, owners, xhi, xlo):
    full = None
    for k, value in enumerate(picked):
        part = dot3(value, xhi[k], xlo[k], ((1,), (1,)))
        full = part if full is None else full + part
    mine = owner_mask(owners, full.shape[0])
    return jnp.sum(jnp.where(mine, full, 0.0), axis=0, keepdims=True)


def send_kernel(owned, xhi, xlo, labels, send, *, geo, nblk):
    owners = geo.owners(False)
    for k, value in enumerate(contributions(owned, owners, xhi, xlo, nblk, geo.planes)):
        send[:, pl.ds(k * LANES, LANES)] = value
    send[:, pl.ds(nblk * LANES, LANES)] = labels[...]


def coarse_kernel(*refs, geo, nblk, peers):
    parts = refs[:peers]
    xhi, xlo, out = refs[peers:]
    owners = geo.owners(False)
    values = [
        jnp.concatenate([part[:, pl.ds(k * LANES, LANES)] for part in parts], axis=0)
        for k in range(nblk + 1)
    ]
    own_labels = parts[0][:, pl.ds(nblk * LANES, LANES)]
    picked = pick_columns(values[:nblk], values[nblk], own_labels, nblk)
    solved = solve_rows(picked, owners, xhi, xlo)
    out[pl.ds(0, 1), :] = solved[:, : geo.lanes]
    out[pl.ds(1, 1), :] = solved[:, geo.lanes :]


def rise(solved, state, consts, out, scratch, geo):
    res, inv, cur_in, resm, invm, curm_in, gref = state
    eig, mref, tref, pref = consts
    cur, curm, tmp, tmpm, step, stepm, low, turned = scratch
    y_hi = mref[MASK_Y_HI : MASK_Y_HI + 1, :] > 0.5
    z_hi = mref[MASK_Z_HI : MASK_Z_HI + 1, :] > 0.5
    xs = geo.wy * geo.cz
    levels = []
    for base, ceil in solved:
        upper = jnp.where(y_hi, roll(base, -geo.cz), ceil)
        flat = [base, upper]
        levels.append([flat, [roll(v, -xs) for v in flat]])
    low_half = mref[NEXT_Z : NEXT_Z + 1, :] > 0.5
    for a in range(NC):
        for b in range(NC):
            flat = [levels[zb][a][b] for zb in range(3)]
            deep = [
                jnp.where(z_hi, roll(flat[zb], -1), roll(flat[(zb + 1) % 3], geo.cz - 1))
                for zb in range(3)
            ]
            for c, value in enumerate((flat, deep)):
                row = pl.ds((a * NC + b) * SUB + c, 1)
                wide_store(low, 0, row, geo, value[1])
                wide_store(low, 1, row, geo, jnp.where(low_half, value[2], value[0]))
    prolong_add(low, curm_in, curm, tref, geo, NM, NC, UP_C, "pz4")
    operate = functools.partial(apply_middle, gref=gref, tref=tref, geo=geo)
    next_smooth(resm, invm, curm, stepm, tmpm, mref, geo, MID, scales(eig, 1), operate)
    prolong_add(curm, cur_in, cur, tref, geo, NF, NM, UP_F, "pz8")
    operate = functools.partial(apply_fine, gref=gref, tref=tref, pref=pref, geo=geo)
    next_smooth(res, inv, cur, step, tmp, mref, geo, FINE, scales(eig, 0), operate)
    words = NF**3 // LANES
    for ch in range(geo.chunks):
        for blk in range(words):
            turned[pl.ds(ch * LANES, LANES), pl.ds(blk * LANES, LANES)] = cur[
                geo.mid, ch, pl.ds(blk * LANES, LANES), :
            ].T
    my = lax.axis_index("gx") * geo.gy + lax.axis_index("gy")
    out[...] = turned[pl.ds(pl.multiple_of(my * geo.ne, SUB), geo.ne), :]


def up_kernel(*refs, geo):
    blocks = [(ref[0:1, :], ref[1:2, :]) for ref in refs[:3]]
    rest = refs[3:]
    rise(blocks, rest[:7], rest[7:11], rest[11], rest[12:], geo.window(2, 0))


def finish_kernel(owned, xhi, xlo, labels, *refs, geo, nblk):
    owners = geo.owners(True)
    values = contributions(owned, owners, xhi, xlo, nblk, labels.shape[0])
    names = labels[...]
    picked = pick_columns(values, names, names, nblk)
    solved = solve_rows(picked, owners, xhi, xlo)
    near = geo.window(2, 0)
    tops = solved[:, geo.nz * geo.lanes :]
    blocks = [
        (solved[:, zb * geo.lanes : (zb + 1) * geo.lanes], roll(tops, geo.cz * zb))
        for zb in range(3)
    ]
    rise(blocks, refs[:7], refs[7:11], refs[11], refs[12:], near)


def holds_all(gx, gy, gz, cy, cz):
    nodes = gx * gy * gz * cy * cz * NF**3
    return 3 <= gz <= gy * cy and nodes * 4 <= MAX_EVERYWHERE


def on_device(residual_in, geometry, eig_top, coarse_rows, block_ids, sizes, everywhere):
    gx, gy, gz = sizes
    cx, cy, cz = residual_in.shape[:3]
    nblk = coarse_rows.shape[3]
    geo = Geo(gx, gy, cy, cz, 3)
    if everywhere:
        geo = geo.window(gz)
    ok = cx == 1 and cz % SUB == 0 and LANES % geo.ne == 0 and geo.lanes % LANES == 0
    ok = ok and all(v & (v - 1) == 0 for v in (geo.ne, cz, geo.wy))
    if not ok or coarse_rows.shape[4] != LANES or geo.planes % SUB:
        raise ValueError("block shape")
    f32 = jnp.float32
    vmem = pl.BlockSpec(memory_space=pltpu.VMEM)
    smem = pl.BlockSpec(memory_space=pltpu.SMEM)
    half, cores = geo.half, geo.cores
    slots = (cy + 1) * cz
    prow = NF**3 // LANES * geo.ne + SUB

    def shape(dims, kind=f32):
        return jax.ShapeDtypeStruct(dims, kind)

    def call(body, specs, outs, scratch, *operands, extra=()):
        kept = list(operands) + list(outs) + list(scratch)
        total = sum(math.prod(a.shape) * a.dtype.itemsize for a in kept)
        return pl.pallas_call(
            body,
            out_shape=list(outs),
            in_specs=specs,
            out_specs=[vmem] * len(outs),
            scratch_shapes=[pltpu.VMEM(a.shape, a.dtype) for a in scratch] + list(extra),
            compiler_params=pltpu.CompilerParams(
                vmem_limit_bytes=min(total + (3 << 20), 60 << 20)
            ),
        )(*operands)

    def rank(ix, ih, core):
        return (ix % gx) * gy + (ih % half) * cores + core

    def across_chips(value):
        parts = [value]
        for dx in range(gx):
            for dh in range(half):
                if dx or dh:
                    pairs = [
                        (rank(ix + dx, ih + dh, core), rank(ix, ih, core))
                        for ix in range(gx)
                        for ih in range(half)
                        for core in range(cores)
                    ]
                    parts.append(lax.ppermute(value, ("gx", "gy"), pairs))
        return parts

    def between_cores(value):
        if cores == 1:
            return value
        return lax.ppermute(value, "gy", [(i, i ^ 1) for i in range(gy)])

    hbm = pl.BlockSpec(memory_space=pltpu.HBM)
    factor = coarse_rows.reshape(cy + 1, cz, nblk, LANES).transpose(0, 2, 1, 3)
    part = shape(((nblk + 1) // 2 * cz, LANES))
    block, factor, keep, give, scale = call(
        functools.partial(pack_kernel, geo=geo),
        [hbm] * 5,
        [shape((prow, LANES)), shape((cy * nblk * cz, LANES)), part, part, shape((SUB, LANES))],
        [shape(geometry.shape), jax.ShapeDtypeStruct(block_ids.shape, block_ids.dtype)],
        *[
            pltpu.with_memory_space_constraint(value, pltpu.HBM)
            for value in (
                residual_in.reshape(geo.ne, NF**3),
                geometry,
                factor.reshape(slots * nblk, LANES),
                block_ids,
                eig_top,
            )
        ],
        extra=[pltpu.SMEM((2,), f32), pltpu.SemaphoreType.DMA((NF**3 // LANES + 6,))],
    )
    marks = [call(mark_kernel, [vmem], [shape((SUB, LANES))], [], scale)[0] for _ in range(2)]

    def from_block(value, offset):
        return lax.ppermute(value, "gz", [((i + offset) % gz, i) for i in range(gz)])

    def along_z(value):
        order = list(range(2, geo.nz - 1)) + [-1, 1]
        got = {offset: from_block(value, offset) for offset in order}
        got[0] = value
        return jnp.concatenate([got[offset] for offset in sorted(got)], axis=0)

    taken = lax.ppermute(give, "gy", [(gy - 1, gy - 2)])
    keep = jnp.where(lax.axis_index("gy") == gy - 1, keep, taken)
    factor = jnp.concatenate([factor, keep], axis=0)
    column = along_z(block)
    if everywhere:
        factor = along_z(factor)
    own = jnp.stack(across_chips(column))
    par = between_cores(own)
    factor_own = across_chips(factor)

    masks = jnp.asarray(geo.masks())
    table = jnp.asarray(TABLE)
    planes = jnp.asarray(PLANES)
    count = geo.planes * (geo.nz if everywhere else 1)
    width = ((geo.nz if everywhere else 1) + 1) * geo.lanes
    near = geo.window(2, 0)

    def field(where, points):
        return shape((where.nz, where.chunks, points * points * SUB, LANES))

    fine, middle, lowest = (field(geo, points) for points in (NF, NM, NC))
    buf = shape((1, 1, NM * NM * SUB, LANES))
    metric = shape((geo.nz, geo.chunks, SUB, LANES))
    fine2, middle2 = (field(near, points) for points in (NF, NM))
    *top, resm, gfac, names = call(
        functools.partial(fine_kernel, geo=geo, prow=prow, everywhere=everywhere),
        [vmem] * 6,
        [fine2] * 3 + [middle, metric, shape((count, LANES))],
        [fine] * 4 + [buf],
        own, par, marks[1], masks, table, planes,
    )
    factor_par = jnp.stack([between_cores(part) for part in factor_own])
    factor_own = jnp.stack(factor_own)
    *merged, owned = call(
        functools.partial(middle_kernel, geo=geo, everywhere=everywhere),
        [vmem] * 5,
        [middle2] * 3
        + [shape((2, geo.chunks, SUB, LANES)), shape((SUB, width))],
        [middle, middle, middle, lowest, buf],
        resm, gfac, marks[0], masks, table,
    )
    wide = shape((nblk, width, LANES), jnp.bfloat16)
    xhi, xlo = call(
        functools.partial(factor_kernel, geo=geo, nblk=nblk, everywhere=everywhere),
        [vmem, vmem],
        [wide, wide],
        [],
        factor_own, factor_par,
    )
    state = (*top, *merged, scale, masks, table, planes)
    kinds = [vmem] * 11
    final = shape((geo.ne, NF**3))
    scratch = [fine2, middle2] * 3 + [field(near, NC), shape((geo.lanes, NF**3))]
    if everywhere:
        (out,) = call(
            functools.partial(finish_kernel, geo=geo, nblk=nblk),
            [vmem] * 4 + kinds,
            [final],
            scratch,
            owned, xhi, xlo, names, *state,
        )
        return out.reshape(cx, cy, cz, NF**3)

    (send,) = call(
        functools.partial(send_kernel, geo=geo, nblk=nblk),
        [vmem] * 4,
        [shape((geo.planes, (nblk + 1) * LANES))],
        [],
        owned, xhi, xlo, names,
    )
    parts = [send] + [from_block(send, offset) for offset in range(1, gz)]
    (solved,) = call(
        functools.partial(coarse_kernel, geo=geo, nblk=nblk, peers=gz),
        [vmem] * (gz + 2),
        [shape((SUB, geo.lanes))],
        [],
        *parts, xhi, xlo,
    )
    (out,) = call(
        functools.partial(up_kernel, geo=geo),
        [vmem] * 3 + kinds,
        [final],
        scratch,
        from_block(solved, -1), solved, from_block(solved, 1), *state,
    )
    return out.reshape(cx, cy, cz, NF**3)


def solution(mesh):
    sizes = tuple(mesh.shape[name] for name in ("gx", "gy", "gz"))
    in_specs = (
        P("gx", "gy", "gz", None),
        P(None, "gx", "gy", "gz"),
        P(),
        P("gx", "gy", "gz", None, None),
        P("gx", "gy", "gz", None),
    )
    out_specs = P("gx", "gy", "gz", None)

    def program(residual_in, geometry, eig_top, coarse_rows, block_ids):
        gx, gy, gz = sizes
        cy, cz = residual_in.shape[1] // gy, residual_in.shape[2] // gz
        everywhere = holds_all(gx, gy, gz, cy, cz)

        def body(*blocks):
            return on_device(*blocks, sizes=sizes, everywhere=everywhere)

        step = jax.shard_map(
            body, mesh=mesh, in_specs=in_specs, out_specs=out_specs, check_vma=False
        )
        return step(residual_in, geometry, eig_top, coarse_rows, block_ids)

    return program
```
